32 devices in a mesh: rows: 8 (over z, y), protos: 4 (over x, core).
Axes of the slice: x: 2, y: 2, z: 4, core: 2. Of those that a mesh axis runs over, the one named last changes fastest.
Arguments:
- features: bfloat16 [3072, 256], P('rows', 'protos'), may hold values from -12 to 12
- prototypes: bfloat16 [65536, 256], P('protos', 'rows'), may hold values from -8 to 8
- masked_index: int32 [1536], P('rows'), may hold values from 0 to 383
Outputs:
- targets: bfloat16 [1536, 65536], P('rows', 'protos')
The draws below stay inside these ranges and needn't reach their ends.
Inputs may be any that keep to these rules, and one draw needn't show every extreme that they name: Row r of the whole takes patch (r // 192) * 384 + masked_index[r] of features.
All inputs are finite; a program needn't handle non-finite values.
Results may differ from the reference program's by a relative error of at most 0.001.
Values may be sent and summed in bfloat16 or wider, within the bound.
A program may use at most 64 MiB of HBM per device.

```python
import jax
import jax.numpy as jnp
from jax import lax

D = 256
K = 65536
MASKED_DEV = 192
ITERS = 3
PATCH_DEV = 384
MASKED = 1536
PATCHES = 3072


def common_directions(key):
    return jax.random.normal(jax.random.fold_in(key, 7), (16, D), jnp.float32)


def draw_features(key, part):
    directions = common_directions(key)
    own_key = jax.random.fold_in(key, 41)
    first, second, third, fourth = jax.random.split(own_key, 4)
    groups = PATCHES // PATCH_DEV
    shifts = jax.random.normal(second, (groups, D), jnp.float32)
    amount = jax.random.uniform(third, (groups, 1), jnp.float32, 0.2, 1.0)
    picked = jax.random.randint(fourth, (groups,), 0, 16)
    aligned = 0.7 * jnp.take(directions, picked, axis=0)
    base = jax.random.normal(first, (PATCHES, D), jnp.float32)
    offset = jnp.repeat(shifts * amount + aligned, PATCH_DEV, axis=0)
    return jnp.clip(base + offset, -12.0, 12.0).astype(jnp.bfloat16)


def draw_prototypes(key, part):
    directions = common_directions(key)
    own_key = jax.random.fold_in(key, 43)
    block_ids = jnp.arange(K, dtype=jnp.int32) * 16 // K
    aligned = 0.6 * jnp.take(directions, block_ids, axis=0)
    base = jax.random.normal(own_key, (K, D), jnp.float32)
    return jnp.clip(base + aligned, -8.0, 8.0).astype(jnp.bfloat16)


def touch_ends(values, stream_key, smallest, largest):
    index_at = [jax.random.randint(jax.random.fold_in(stream_key, axis), (), 0, length) for axis, length in enumerate(values.shape)]
    widest = values.shape.index(max(values.shape))
    neighbour = index_at[:widest] + [(index_at[widest] + 1) % values.shape[widest]] + index_at[widest + 1:]
    return values.at[tuple(index_at)].set(smallest).at[tuple(neighbour)].set(largest)


def setup_inputs(seed: int = 0) -> dict:
    seeds = jax.random.split(jax.random.key(seed), 4)
    return {
        "features": draw_features(jax.random.fold_in(seeds[3], 71), 0),
        "prototypes": draw_prototypes(jax.random.fold_in(seeds[3], 71), 0),
        "masked_index": touch_ends(jax.random.randint(seeds[2], (MASKED,), 0, PATCH_DEV), jax.random.fold_in(seeds[2], 1), 0, PATCH_DEV - 1).astype(jnp.int32),
    }


TEMP = 0.07
EPS = 1e-06

def reference(features, prototypes, masked_index):
    owner = jnp.arange(MASKED, dtype=jnp.int32) // MASKED_DEV
    rowids = (owner * PATCH_DEV + masked_index).astype(jnp.int32)
    selected = jnp.take(features, rowids, axis=0)
    feat_scale = lax.rsqrt(lax.optimization_barrier(jnp.sum(jnp.square(selected.astype(jnp.float32)), axis=1)) + EPS)
    proto_scale = lax.rsqrt(lax.optimization_barrier(jnp.sum(jnp.square(prototypes.astype(jnp.float32)), axis=1)) + EPS)
    blocks = MASKED // MASKED_DEV
    protos_t = prototypes.T

    def weights_of(index):
        start = (index * MASKED_DEV).astype(jnp.int32)
        part = lax.dynamic_slice_in_dim(selected, start, MASKED_DEV, 0)
        scale = lax.dynamic_slice_in_dim(feat_scale, start, MASKED_DEV, 0)
        raw = jnp.dot(part, protos_t, preferred_element_type=jnp.float32)
        return jnp.exp(raw * scale[:, None] * proto_scale[None, :] / TEMP)

    def first_pass(total, index):
        return (total + lax.optimization_barrier(jnp.sum(weights_of(index), axis=0)), None)
    indices = jnp.arange(blocks, dtype=jnp.int32)
    col_mass, unused = lax.scan(first_pass, jnp.zeros((K,), jnp.float32), indices)
    for step in range(ITERS):
        col_scale = 1.0 / (K * col_mass)
        if step + 1 < ITERS:

            def middle(total, index):
                block = weights_of(index)
                row_mass = jnp.dot(block, col_scale, precision=lax.Precision.HIGHEST)
                row_scale = 1.0 / (MASKED * row_mass)
                return (total + jnp.dot(row_scale, block, precision=lax.Precision.HIGHEST), None)
            col_mass, unused = lax.scan(middle, jnp.zeros((K,), jnp.float32), indices)
        else:

            def final(carry, index):
                block = weights_of(index)
                row_mass = jnp.dot(block, col_scale, precision=lax.Precision.HIGHEST)
                row_scale = 1.0 / (MASKED * row_mass)
                result = float(K) * float(MASKED) * row_scale[:, None] * block * col_scale[None, :]
                return (carry, result.astype(jnp.bfloat16))
            unused, outputs = lax.scan(final, jnp.zeros((), jnp.float32), indices)
    return outputs.reshape(MASKED, K)
```

```python
import functools

import jax
import jax.numpy as jnp
from jax import lax
from jax.experimental import pallas as pl
from jax.experimental.pallas import tpu as pltpu
from jax.sharding import PartitionSpec as P

ITERS = 3


TEMP = 0.07
EPS = 1e-06
LOG2E = 1.4426950408889634
UP, DOWN, ACROSS = 0, 1, 2
LEAD = 6
SPLIT = 2
EARLY = (5, 10)
LAG = 4
BLOCK = 128


def kernel(
    n_rows, n_protos, masked, protos_all,
    feat_ref, proto_ref, index_ref, out_ref,
    feat_in, index, onehot, picks, patches, pair, chosen, lane_scale, feat_scale, full, weights,
    acc, row_out, row_in, mass_out, mass_in, row_scale, out_scale, scales,
    in_sem, own_sem, pick_send, pick_recv, patch_send, patch_recv, send, recv, direct_send,
    row_send, row_recv, mass_send, mass_recv, scale_send, scale_recv,
):
    r, p = lax.axis_index("rows"), lax.axis_index("protos")
    z, y = r // 2, lax.rem(r, 2)
    nz = n_rows // 2
    other = z * 2 + 1 - y
    dim, total = proto_ref.shape
    width = total // n_rows
    chunks = n_rows * SPLIT
    span = total // chunks
    rows = index_ref.shape[1]
    fdim = feat_ref.shape[0]
    lanes = rows * n_rows
    odd = y == 1
    both = jnp.logical_and
    no = jnp.logical_not
    mesh_id = pl.DeviceIdType.MESH

    def where(src, c):
        return full.at[c, pl.ds(pl.multiple_of(src * dim, dim), dim)]

    def own_copy(c):
        return pltpu.make_async_copy(
            proto_ref.at[:, pl.ds(pl.multiple_of(c * span, span), span)], where(r, c), own_sem.at[c]
        )

    def early(c):
        hit = c == EARLY[0]
        for e in EARLY[1:]:
            hit = jnp.logical_or(hit, c == e)
        return hit

    def owner(c):
        return c // SPLIT

    def plane(c):
        return c // (2 * SPLIT)

    def remote(src, dst, send_sem, recv_sem, **device):
        return pltpu.make_async_remote_copy(
            src_ref=src, dst_ref=dst, send_sem=send_sem, recv_sem=recv_sem,
            device_id=device, device_id_type=mesh_id,
        )

    def block_copy(way, src, c):
        target = {UP: r + 2, DOWN: r - 2, ACROSS: other}[way]
        return remote(where(src, c), where(src, c), send.at[way, src, c], recv.at[src, c], rows=target)

    def when(condition, action):
        @pl.when(condition)
        def _():
            action()

    def each(count, body):
        def step(i, carry):
            body(i)
            return carry

        lax.fori_loop(0, count, step, 0)

    def goes_up(c, on_line):
        return both(z < nz - 1, plane(c) != z + 1 if on_line else owner(c) != r + 2)

    def goes_down(c, on_line):
        return both(z > 0, plane(c) != z - 1 if on_line else owner(c) != r - 2)

    def direct_copy(step, c):
        target = lax.rem(r + 2 * step, n_rows)
        chunk = target // 2 * (2 * SPLIT) + c
        return remote(
            where(r, chunk), where(r, chunk), direct_send.at[step, c], recv.at[r, chunk], rows=target
        )

    def pick_copy(step):
        return remote(
            picks.at[r], picks.at[r], pick_send.at[step], pick_recv.at[r], rows=lax.rem(r + step, n_rows)
        )

    def pick_from(src):
        return remote(picks.at[src], picks.at[src], pick_send.at[0], pick_recv.at[src], rows=other)

    def patch_copy(step, src):
        part = patches.at[pl.ds(pl.multiple_of(src * fdim, fdim), fdim)]
        return remote(
            part, part, patch_send.at[step], patch_recv.at[src], protos=lax.rem(p + step, n_protos)
        )

    def row_copy(it, step):
        return remote(
            row_out.at[it], row_in.at[it, step], row_send.at[it, step], row_recv.at[it, step],
            protos=lax.rem(p + step, n_protos),
        )

    def mass_copy(it, step):
        return remote(
            mass_out.at[it], mass_in.at[it, step], mass_send.at[it, step], mass_recv.at[it, step],
            rows=lax.rem(r + step, n_rows),
        )

    def scale_copy(step, src):
        return remote(
            scales.at[src], scales.at[src], scale_send.at[step], scale_recv.at[src],
            rows=lax.rem(r + step, n_rows),
        )

    feat_load = pltpu.make_async_copy(feat_ref, feat_in, in_sem.at[0])
    index_load = pltpu.make_async_copy(index_ref, index, in_sem.at[1])
    feat_load.start()
    index_load.start()
    each(chunks, lambda c: own_copy(c).start())

    barrier = pltpu.get_barrier_semaphore()
    for step in range(1, n_rows):
        pl.semaphore_signal(
            barrier, inc=1, device_id={"rows": lax.rem(r + step, n_rows)}, device_id_type=mesh_id
        )
    for step in range(1, n_protos):
        pl.semaphore_signal(
            barrier, inc=1, device_id={"protos": lax.rem(p + step, n_protos)}, device_id_type=mesh_id
        )

    onehot[...] = jnp.zeros_like(onehot)
    index_load.wait()
    hits = lax.broadcasted_iota(jnp.int32, (onehot.shape[0], rows), 0) == index[...]
    onehot[:, :rows] = hits.astype(jnp.float32).astype(jnp.bfloat16)
    feat_load.wait()
    picked = jnp.dot(feat_in[...], onehot[...], preferred_element_type=jnp.float32)
    picked = jnp.where(odd, pltpu.roll(picked, 2 * BLOCK - rows, 1), picked)
    picks[r] = picked.astype(jnp.bfloat16)
    acc[...] = jnp.zeros_like(acc)
    each(chunks, lambda c: own_copy(c).wait())

    pl.semaphore_wait(barrier, n_rows + n_protos - 2)

    for step in range(1, n_rows):
        pick_copy(step).start()

    def begin(c):
        when(both(owner(c) == other, c >= 0), lambda: block_copy(ACROSS, r, c).start())

    each(chunks, begin)
    for step in range(1, nz):
        for c in range(2 * SPLIT):
            direct_copy(step, c).start()

    def send_own(c):
        when(goes_up(c, True), lambda: block_copy(UP, r, c).start())
        when(goes_down(c, True), lambda: block_copy(DOWN, r, c).start())
        when(owner(c) != other, lambda: block_copy(ACROSS, r, c).start())

    each(LEAD, send_own)

    for step in range(1, n_rows):
        pick_from(lax.rem(r + step, n_rows)).wait_recv()
    mine = pl.ds(pl.multiple_of(p * fdim, fdim), fdim)
    for j in range(nz):
        at = 3 * BLOCK * j
        patches[mine, at:at + BLOCK] = picks[2 * j, :, :BLOCK]
        patches[mine, at + BLOCK:at + 2 * BLOCK] = (
            picks[2 * j, :, BLOCK:].astype(jnp.float32) + picks[2 * j + 1, :, :BLOCK].astype(jnp.float32)
        ).astype(jnp.bfloat16)
        patches[mine, at + 2 * BLOCK:at + 3 * BLOCK] = picks[2 * j + 1, :, BLOCK:]
    for step in range(1, n_protos):
        patch_copy(step, p).start()

    def relay(step):
        src = lax.rem(r + 2 * step, n_rows)
        for j in range(SPLIT):
            block_copy(ACROSS, src, other * SPLIT + j).wait_recv()
            block_copy(ACROSS, src, other * SPLIT + j).start()
        for j in range(SPLIT):
            block_copy(ACROSS, src, r * SPLIT + j).wait_recv()

    for step in range(1, nz):
        relay(step)

    for step in range(1, n_protos):
        patch_copy(step, lax.rem(p + step, n_protos)).wait_recv()
    pair[...] = patches[:, pl.ds(pl.multiple_of(z * (2 * rows), 2 * rows), 2 * rows)].T
    chosen[...] = pair[pl.ds(pl.multiple_of(y * rows, rows), rows), :]
    wide = chosen[...].astype(jnp.float32)
    scale = lax.rsqrt(jnp.sum(wide * wide, axis=1, keepdims=True) + EPS)
    feat_scale[...] = jnp.broadcast_to(scale * (LOG2E / TEMP), feat_scale.shape)
    for t in range(lanes // BLOCK):
        wide = patches[:, t * BLOCK:(t + 1) * BLOCK].astype(jnp.float32)
        scale = lax.rsqrt(jnp.sum(wide * wide, axis=0, keepdims=True) + EPS)
        lane_scale[:, t * BLOCK:(t + 1) * BLOCK] = scale * (LOG2E / TEMP)
    for step in range(nz):
        src = lax.rem(other + 2 * step, n_rows)
        for j in range(SPLIT):
            block_copy(ACROSS, src, r * SPLIT + j).wait_recv()

    def turned(column):
        return jnp.broadcast_to(column, (BLOCK, BLOCK)).T[:1]

    def add_rows(value, col_mass, tile):
        col_scale = 1.0 / (protos_all * col_mass)
        scaled = (value * col_scale).reshape(BLOCK // 8, 8, lanes)
        acc[...] += jnp.sum(scaled, axis=0)
        return col_scale

    def make_weights(half):
        def body(i):
            tile = half * (width // BLOCK // 2) + i
            per = span // BLOCK
            within = pl.ds(pl.multiple_of(lax.rem(tile, per) * BLOCK, BLOCK), BLOCK)
            block = full[r * SPLIT + tile // per, :, within].T
            wide = block.astype(jnp.float32)
            proto_scale = lax.rsqrt(jnp.sum(wide * wide, axis=1, keepdims=True) + EPS)
            raw = jnp.dot(block, patches[...], preferred_element_type=jnp.float32)
            value = jnp.exp2(raw * lane_scale[...] * proto_scale)
            weights[pl.ds(pl.multiple_of(tile * BLOCK, BLOCK), BLOCK)] = value
            add_rows(value, jnp.sum(value, axis=1, keepdims=True), tile)
            scales[r, 1, :, pl.ds(pl.multiple_of(tile * BLOCK, BLOCK), BLOCK)] = turned(proto_scale)

        each(width // BLOCK // 2, body)

    def one_pass(it):
        def body(tile):
            at = pl.ds(pl.multiple_of(tile * BLOCK, BLOCK), BLOCK)
            value = weights[at]
            col_mass = jnp.sum(value * row_scale[...], axis=1, keepdims=True)
            col_scale = add_rows(value, col_mass, tile)
            if it == ITERS - 1:
                scales[r, 0, :, at] = turned(col_scale)

        each(width // BLOCK, body)

    def give_rows(it):
        row_out[it] = jnp.sum(acc[...], axis=0, keepdims=True)
        acc[...] = jnp.zeros_like(acc)
        for step in range(1, n_protos):
            row_copy(it, step).start()

    def give_mass(it):
        mass = row_out[it]
        for step in range(1, n_protos):
            row_copy(it, step).wait_recv()
            mass = mass + row_in[it, step]
        mass_out[it] = mass
        for step in range(1, n_rows):
            mass_copy(it, step).start()

    def take_mass(it):
        mass = mass_out[it]
        for step in range(1, n_rows):
            mass_copy(it, step).wait_recv()
            mass = mass + mass_in[it, step]
        row_scale[...] = 1.0 / (masked * mass)

    def next_pass(it):
        take_mass(it - 1)
        one_pass(it)
        if it == ITERS - 1:
            for step in range(1, n_rows):
                scale_copy(step, r).start()
        give_rows(it)

    def settle():
        take_mass(ITERS - 1)
        at = lax.broadcasted_iota(jnp.int32, (rows, lanes), 1)
        row = lax.broadcasted_iota(jnp.int32, (rows, lanes), 0) + r * rows
        found = jnp.where(at == row, jnp.broadcast_to(row_scale[...], (rows, lanes)), 0.0)
        found = jnp.sum(found, axis=1, keepdims=True) * (protos_all * masked)
        out_scale[...] = jnp.broadcast_to(found, out_scale.shape)
        for step in range(1, n_rows):
            scale_copy(step, lax.rem(r + step, n_rows)).wait_recv()

    def make_output(c):
        tile = min(512, span)
        for t in range(span // tile):
            block = full[c, :, t * tile:(t + 1) * tile]
            raw = jnp.dot(chosen[...], block, preferred_element_type=jnp.float32)
            at = pl.ds(pl.multiple_of(lax.rem(c, SPLIT) * span + t * tile, tile), tile)
            value = jnp.exp2(raw * feat_scale[:, :1] * scales[owner(c), 1, :, at])
            value = out_scale[:, :1] * value * scales[owner(c), 0, :, at]
            out_ref[c, :, t * tile:(t + 1) * tile] = value.astype(jnp.bfloat16)

    stages = {
        0: lambda: make_weights(0),
        1: lambda: (make_weights(1), give_rows(0)),
        2: lambda: give_mass(0),
        4: lambda: next_pass(1),
        5: lambda: give_mass(1),
        7: lambda: next_pass(2),
        8: lambda: give_mass(2),
        10: settle,
    }
    first = 11
    pace = 4

    def beside(c):
        src = other
        when(owner(c) != r, lambda: block_copy(ACROSS, src, c).wait_recv())
        when(both(early(c), goes_up(c, False)), lambda: block_copy(UP, src, c).start())
        when(both(early(c), goes_down(c, False)), lambda: block_copy(DOWN, src, c).start())

    def ways(d):
        return (
            (DOWN, z + d, goes_down, z + d < nz),
            (UP, z - d, goes_up, z - d >= 0),
        )

    def line(c, d):
        for way, ahead, more, there in ways(d):
            src = ahead * 2 + y

            @pl.when(there)
            def _():
                when(plane(c) != z, lambda: block_copy(ACROSS, src, c).wait_recv())
                when(more(c, True), lambda: block_copy(way, src, c).start())
                when(
                    both(no(early(c)), owner(c) != other), lambda: block_copy(ACROSS, src, c).start()
                )

    def far_line(c, d):
        for way, ahead, more, there in ways(d):
            src = ahead * 2 + 1 - y

            @pl.when(there)
            def _():
                when(owner(c) != r, lambda: block_copy(ACROSS, src, c).wait_recv())
                when(both(early(c), more(c, False)), lambda: block_copy(way, src, c).start())

    def drain(c):
        for src_z in range(nz):
            for src_y in range(2):
                src = src_z * 2 + src_y
                on_line = src_y == y
                up = jnp.where(on_line, goes_up(c, True), both(early(c), goes_up(c, False)))
                down = jnp.where(on_line, goes_down(c, True), both(early(c), goes_down(c, False)))
                kept = both(src_z != z, both(early(c), owner(c) != other))
                when(both(up, src_z <= z), lambda: block_copy(UP, src, c).wait_send())
                when(both(down, src_z >= z), lambda: block_copy(DOWN, src, c).wait_send())
                when(both(on_line, no(kept)), lambda: block_copy(ACROSS, src, c).wait_send())

    def done_by(i):
        return jnp.clip(jnp.minimum((i - first + 1) * pace, i - nz + 2), 0, chunks)

    def step_of(i, carry):
        when(i + LEAD < chunks, lambda: send_own(i + LEAD))
        when(i < chunks, lambda: beside(i))
        for d in range(1, nz):
            c = i - (d - 1)
            when(both(c >= 0, c < chunks), lambda: line(c, d))
        for d in range(1, nz):
            c = i - d
            when(both(both(c >= 0, c < chunks), early(c)), lambda: far_line(c, d))
        last = i - (nz - 1)

        @pl.when(both(last >= 0, no(early(last))))
        def _():
            for d in range(1, nz):
                far_line(last, d)

        for at, stage in stages.items():
            when(i == at, stage)

        def output(c, carry):
            make_output(c)
            return carry

        lax.fori_loop(done_by(i - 1), done_by(i), output, 0)
        when(last >= LAG, lambda: drain(last - LAG))
        return carry

    steps = chunks + nz - 1
    lax.fori_loop(0, steps, step_of, 0)

    for step in range(1, n_rows):
        pick_copy(step).wait_send()
        scale_copy(step, r).wait_send()
    for step in range(1, nz):
        for c in range(2 * SPLIT):
            direct_copy(step, c).wait_send()
    for step in range(1, n_protos):
        patch_copy(step, p).wait_send()
    for it in range(ITERS):
        for step in range(1, n_rows):
            mass_copy(it, step).wait_send()
        for step in range(1, n_protos):
            row_copy(it, step).wait_send()

    def rest(i, carry):
        drain(i)
        return carry

    lax.fori_loop(chunks - LAG, chunks, rest, 0)


def finish(blocks_ref, out_ref, out_sem):
    count, rows, span = blocks_ref.shape
    copies = [
        pltpu.make_async_copy(
            blocks_ref.at[c], out_ref.at[:, c * span:(c + 1) * span], out_sem.at[c]
        )
        for c in range(count)
    ]
    for copy in copies:
        copy.start()
    for copy in copies:
        copy.wait()


def with_kernel(n_rows, n_protos, features, prototypes, masked_index):
    rows = masked_index.shape[0]
    dim, total = prototypes.shape[1], prototypes.shape[0]
    fdim, patches = features.shape[1], features.shape[0]
    width = total // n_rows
    chunks = n_rows * SPLIT
    span = total // chunks
    lanes = rows * n_rows
    depth = fdim * n_protos
    masked = float(lanes)
    protos_all = float(total * n_protos)
    f32, bf16, dma = jnp.float32, jnp.bfloat16, pltpu.SemaphoreType.DMA
    vmem = pl.BlockSpec(memory_space=pltpu.VMEM)
    anywhere = pl.BlockSpec(memory_space=pl.ANY)
    blocks = pl.pallas_call(
        functools.partial(kernel, n_rows, n_protos, masked, protos_all),
        out_shape=jax.ShapeDtypeStruct((chunks, rows, span), bf16),
        in_specs=[pl.BlockSpec(memory_space=pltpu.HBM)] * 3,
        out_specs=vmem,
        scratch_shapes=[
            pltpu.VMEM((fdim, patches), bf16),
            pltpu.VMEM((1, rows), jnp.int32),
            pltpu.VMEM((patches, 2 * BLOCK), bf16),
            pltpu.VMEM((n_rows, fdim, 2 * BLOCK), bf16),
            pltpu.VMEM((depth, lanes), bf16),
            pltpu.VMEM((2 * rows, depth), bf16),
            pltpu.VMEM((rows, depth), bf16),
            pltpu.VMEM((1, lanes), f32),
            pltpu.VMEM((rows, BLOCK), f32),
            pltpu.VMEM((chunks, dim * n_rows, span), bf16),
            pltpu.VMEM((width, lanes), f32),
            pltpu.VMEM((8, lanes), f32),
            pltpu.VMEM((ITERS, 1, lanes), f32),
            pltpu.VMEM((ITERS, n_protos, 1, lanes), f32),
            pltpu.VMEM((ITERS, 1, lanes), f32),
            pltpu.VMEM((ITERS, n_rows, 1, lanes), f32),
            pltpu.VMEM((1, lanes), f32),
            pltpu.VMEM((rows, BLOCK), f32),
            pltpu.VMEM((n_rows, 2, 1, width), f32),
            dma((2,)),
            dma((chunks,)),
            dma((n_rows,)),
            dma((n_rows,)),
            dma((n_protos,)),
            dma((n_protos,)),
            dma((3, n_rows, chunks)),
            dma((n_rows, chunks)),
            dma((n_rows // 2, 2 * SPLIT)),
            dma((ITERS, n_protos)),
            dma((ITERS, n_protos)),
            dma((ITERS, n_rows)),
            dma((ITERS, n_rows)),
            dma((n_rows,)),
            dma((n_rows,)),
        ],
        compiler_params=pltpu.CompilerParams(
            collective_id=0, has_side_effects=True, vmem_limit_bytes=56 * 1024 * 1024
        ),
    )(features.T, prototypes.T, masked_index[None, :])
    return pl.pallas_call(
        finish,
        out_shape=jax.ShapeDtypeStruct((rows, total), bf16),
        in_specs=[vmem],
        out_specs=anywhere,
        scratch_shapes=[dma((chunks,))],
        compiler_params=pltpu.CompilerParams(vmem_limit_bytes=4 * 1024 * 1024),
    )(blocks)


def with_collectives(features, prototypes, masked_index):
    total_protos = float(prototypes.shape[0] * lax.axis_size("protos"))
    chosen = jnp.take(features, masked_index, axis=0)
    patches = lax.all_gather(chosen, "protos", axis=1, tiled=True)
    feat_scale = lax.rsqrt(jnp.sum(jnp.square(patches.astype(jnp.float32)), axis=1) + EPS)
    full = lax.all_gather(prototypes, "rows", axis=1, tiled=True)
    proto_sq = jnp.sum(jnp.square(full.astype(jnp.float32)), axis=1)
    raw = lax.dot_general(
        patches, full, (((1,), (1,)), ((), ())), preferred_element_type=jnp.float32
    )
    proto_scale = lax.rsqrt(proto_sq + EPS)
    weights = jnp.exp(raw * feat_scale[:, None] * proto_scale[None, :] / TEMP)
    total_rows = masked_index.shape[0] * lax.axis_size("rows")
    row_scale = jnp.ones((patches.shape[0],), jnp.float32)
    for step in range(ITERS):
        col_part = jnp.dot(row_scale, weights, precision=lax.Precision.HIGHEST)
        col_scale = 1.0 / (total_protos * lax.psum(col_part, "rows"))
        row_part = jnp.dot(weights, col_scale, precision=lax.Precision.HIGHEST)
        row_scale = 1.0 / (total_rows * lax.psum(row_part, "protos"))
    factor = total_protos * float(total_rows)
    return (factor * row_scale[:, None] * weights * col_scale[None, :]).astype(jnp.bfloat16)


def solution(mesh):
    n_rows, n_protos = mesh.shape["rows"], mesh.shape["protos"]
    in_specs = (P("rows", "protos"), P("protos", "rows"), P("rows"))
    out_specs = P("rows", "protos")

    def on_device(features, prototypes, masked_index):
        fits = (
            n_rows % 2 == 0
            and n_rows == 8
            and n_protos > 1
            and prototypes.shape[1] % 16 == 0
            and features.shape[1] % 16 == 0
            and features.shape[1] * n_protos == prototypes.shape[1] * n_rows
            and 2 * masked_index.shape[0] == 3 * BLOCK
            and prototypes.shape[0] % (n_rows * SPLIT * 512) == 0
        )
        if fits:
            return with_kernel(n_rows, n_protos, features, prototypes, masked_index)
        return with_collectives(features, prototypes, masked_index)

    return jax.shard_map(
        on_device, mesh=mesh, in_specs=in_specs, out_specs=out_specs, check_vma=False
    )
```

```python
import functools

import jax
import jax.numpy as jnp
from jax import lax
from jax.experimental import pallas as pl
from jax.experimental.pallas import tpu as pltpu
from jax.sharding import PartitionSpec as P

ITERS = 3


TEMP = 0.07
EPS = 1e-06
LOG2E = 1.4426950408889634
UP, DOWN, ACROSS = 0, 1, 2
LEAD_Z = (8, 3, 6, 0)
LEAD_Y = 8
SPLIT = 1
EARLY = (4,)
EARLY_AT = 3
LAG = 2
STATS_AT = 0
BLOCK = 128


def kernel(
    n_rows, n_protos, masked, protos_all,
    feat_ref, proto_ref, index_ref, out_ref,
    feat_in, index, onehot, picks, patches, pair, chosen, lane_scale, feat_scale, full, weights,
    acc, row_out, row_in, mass_out, mass_in, row_scale, out_scale, scales,
    in_sem, own_sem, pick_send, pick_recv, patch_send, patch_recv, send, recv, direct_send,
    row_send, row_recv, mass_send, mass_recv, scale_send, scale_recv,
):
    r, p = lax.axis_index("rows"), lax.axis_index("protos")
    z, y = r // 2, lax.rem(r, 2)
    nz = n_rows // 2
    other = z * 2 + 1 - y
    dim, total = proto_ref.shape
    width = total // n_rows
    chunks = n_rows * SPLIT
    span = total // chunks
    rows = index_ref.shape[1]
    fdim = feat_ref.shape[0]
    lanes = rows * n_rows
    odd = y == 1
    both = jnp.logical_and
    no = jnp.logical_not
    mesh_id = pl.DeviceIdType.MESH

    def where(src, c):
        return full.at[c, pl.ds(pl.multiple_of(src * dim, dim), dim)]

    def own_copy(c):
        return pltpu.make_async_copy(
            proto_ref.at[:, pl.ds(pl.multiple_of(c * span, span), span)], where(r, c), own_sem.at[c]
        )

    def early(c):
        hit = c == EARLY[0]
        for e in EARLY[1:]:
            hit = jnp.logical_or(hit, c == e)
        return hit

    def owner(c):
        return c // SPLIT

    def plane(c):
        return c // (2 * SPLIT)

    def remote(src, dst, send_sem, recv_sem, **device):
        return pltpu.make_async_remote_copy(
            src_ref=src, dst_ref=dst, send_sem=send_sem, recv_sem=recv_sem,
            device_id=device, device_id_type=mesh_id,
        )

    def block_copy(way, src, c):
        target = {UP: r + 2, DOWN: r - 2, ACROSS: other}[way]
        return remote(where(src, c), where(src, c), send.at[way, src, c], recv.at[src, c], rows=target)

    def when(condition, action):
        @pl.when(condition)
        def _():
            action()

    def each(count, body):
        def step(i, carry):
            body(i)
            return carry

        lax.fori_loop(0, count, step, 0)

    def goes_up(c, on_line):
        return both(z < nz - 1, plane(c) != z + 1 if on_line else owner(c) != r + 2)

    def goes_down(c, on_line):
        return both(z > 0, plane(c) != z - 1 if on_line else owner(c) != r - 2)

    def direct_copy(step, c):
        target = lax.rem(r + 2 * step, n_rows)
        chunk = target // 2 * (2 * SPLIT) + c
        return remote(
            where(r, chunk), where(r, chunk), direct_send.at[step, c], recv.at[r, chunk], rows=target
        )

    def pick_copy(step):
        return remote(
            picks.at[r], picks.at[r], pick_send.at[step], pick_recv.at[r], rows=lax.rem(r + step, n_rows)
        )

    def pick_from(src):
        return remote(picks.at[src], picks.at[src], pick_send.at[0], pick_recv.at[src], rows=other)

    def patch_copy(step, src):
        part = patches.at[pl.ds(pl.multiple_of(src * fdim, fdim), fdim)]
        return remote(
            part, part, patch_send.at[step], patch_recv.at[src], protos=lax.rem(p + step, n_protos)
        )

    def row_copy(it, step):
        return remote(
            row_out.at[it], row_in.at[it, step], row_send.at[it, step], row_recv.at[it, step],
            protos=lax.rem(p + step, n_protos),
        )

    def mass_copy(it, step):
        return remote(
            mass_out.at[it], mass_in.at[it, step], mass_send.at[it, step], mass_recv.at[it, step],
            rows=lax.rem(r + step, n_rows),
        )

    def scale_copy(step, src):
        return remote(
            scales.at[src], scales.at[src], scale_send.at[step], scale_recv.at[src],
            rows=lax.rem(r + step, n_rows),
        )

    feat_load = pltpu.make_async_copy(feat_ref, feat_in, in_sem.at[0])
    index_load = pltpu.make_async_copy(index_ref, index, in_sem.at[1])
    feat_load.start()
    index_load.start()
    each(chunks, lambda c: own_copy(c).start())

    barrier = pltpu.get_barrier_semaphore()
    for step in range(1, n_rows):
        pl.semaphore_signal(
            barrier, inc=1, device_id={"rows": lax.rem(r + step, n_rows)}, device_id_type=mesh_id
        )
    for step in range(1, n_protos):
        pl.semaphore_signal(
            barrier, inc=1, device_id={"protos": lax.rem(p + step, n_protos)}, device_id_type=mesh_id
        )

    onehot[...] = jnp.zeros_like(onehot)
    index_load.wait()
    hits = lax.broadcasted_iota(jnp.int32, (onehot.shape[0], rows), 0) == index[...]
    onehot[:, :rows] = hits.astype(jnp.float32).astype(jnp.bfloat16)
    feat_load.wait()
    picked = jnp.dot(feat_in[...], onehot[...], preferred_element_type=jnp.float32)
    picked = jnp.where(odd, pltpu.roll(picked, 2 * BLOCK - rows, 1), picked)
    picks[r] = picked.astype(jnp.bfloat16)
    acc[...] = jnp.zeros_like(acc)
    each(chunks, lambda c: own_copy(c).wait())

    pl.semaphore_wait(barrier, n_rows + n_protos - 2)

    for step in range(1, n_rows):
        pick_copy(step).start()

    def begin(c):
        when(both(owner(c) == other, c >= 0), lambda: block_copy(ACROSS, r, c).start())

    each(chunks, begin)
    for apart in range(1, nz):
        for side in (1, -1):
            there = both(z + side * apart >= 0, z + side * apart < nz)
            for c in range(2 * SPLIT):
                when(there, lambda: direct_copy(lax.rem(nz + side * apart, nz), c).start())

    def order(way, k):
        if way == ACROSS:
            swapped = jnp.where(both(k >= EARLY_AT, k <= EARLY_AT + 1), 2 * EARLY_AT + 1 - k, k)
            return jnp.where(z < nz // 2, chunks - 1 - k, swapped)
        return k if way == UP else chunks - 1 - k

    def lead(way):
        behind = z if way == UP else nz - 1 - z
        count = LEAD_Z[nz - 1]
        for at in range(nz - 1):
            count = jnp.where(behind == at, LEAD_Z[at], count)
        return count

    def own_line(way, k):
        c = order(way, k)
        more = (goes_up if way == UP else goes_down)(c, True)
        when(both(k < chunks, more), lambda: block_copy(way, r, c).start())

    def own_across(k):
        c = order(ACROSS, k)
        when(both(k < chunks, owner(c) != other), lambda: block_copy(ACROSS, r, c).start())

    for way in (DOWN, UP):
        each(lead(way), functools.partial(own_line, way))
    each(LEAD_Y, own_across)

    for step in range(1, n_rows):
        pick_from(lax.rem(r + step, n_rows)).wait_recv()
    mine = pl.ds(pl.multiple_of(p * fdim, fdim), fdim)
    for j in range(nz):
        at = 3 * BLOCK * j
        patches[mine, at:at + BLOCK] = picks[2 * j, :, :BLOCK]
        patches[mine, at + BLOCK:at + 2 * BLOCK] = (
            picks[2 * j, :, BLOCK:].astype(jnp.float32) + picks[2 * j + 1, :, :BLOCK].astype(jnp.float32)
        ).astype(jnp.bfloat16)
        patches[mine, at + 2 * BLOCK:at + 3 * BLOCK] = picks[2 * j + 1, :, BLOCK:]
    for step in range(1, n_protos):
        patch_copy(step, p).start()

    def relay():
        for apart in range(1, nz):
            for side in (1, -1):
                ahead = z + side * apart
                src = ahead * 2 + y

                @pl.when(both(ahead >= 0, ahead < nz))
                def _():
                    for j in range(SPLIT):
                        block_copy(ACROSS, src, other * SPLIT + j).wait_recv()
                        block_copy(ACROSS, src, other * SPLIT + j).start()
                    for j in range(SPLIT):
                        block_copy(ACROSS, src, r * SPLIT + j).wait_recv()

    def take_patches():
        for step in range(1, n_protos):
            patch_copy(step, lax.rem(p + step, n_protos)).wait_recv()
        pair[...] = patches[:, pl.ds(pl.multiple_of(z * (2 * rows), 2 * rows), 2 * rows)].T
        chosen[...] = pair[pl.ds(pl.multiple_of(y * rows, rows), rows), :]
        wide = chosen[...].astype(jnp.float32)
        scale = lax.rsqrt(jnp.sum(wide * wide, axis=1, keepdims=True) + EPS)
        feat_scale[...] = jnp.broadcast_to(scale * (LOG2E / TEMP), feat_scale.shape)
        for t in range(lanes // BLOCK):
            wide = patches[:, t * BLOCK:(t + 1) * BLOCK].astype(jnp.float32)
            scale = lax.rsqrt(jnp.sum(wide * wide, axis=0, keepdims=True) + EPS)
            lane_scale[:, t * BLOCK:(t + 1) * BLOCK] = scale * (LOG2E / TEMP)

    def take_own():
        for step in range(nz):
            src = lax.rem(other + 2 * step, n_rows)
            apart = jnp.abs(src // 2 - z)
            for j in range(SPLIT):
                c = r * SPLIT + j
                k = jnp.where(src // 2 > z, order(DOWN, c), c)
                at = jnp.where(early(c), EARLY_AT + apart, k + nz - 1)
                at = jnp.where(apart == 0, order(ACROSS, c), at)
                when(at > STATS_AT, lambda: block_copy(ACROSS, src, c).wait_recv())

    def turned(column):
        return jnp.broadcast_to(column, (BLOCK, BLOCK)).T[:1]

    def add_rows(value, col_mass, tile):
        col_scale = 1.0 / (protos_all * col_mass)
        scaled = (value * col_scale).reshape(BLOCK // 8, 8, lanes)
        acc[...] += jnp.sum(scaled, axis=0)
        return col_scale

    def make_weights(half):
        def body(i):
            tile = half * (width // BLOCK // 2) + i
            per = span // BLOCK
            within = pl.ds(pl.multiple_of(lax.rem(tile, per) * BLOCK, BLOCK), BLOCK)
            block = full[r * SPLIT + tile // per, :, within].T
            wide = block.astype(jnp.float32)
            proto_scale = lax.rsqrt(jnp.sum(wide * wide, axis=1, keepdims=True) + EPS)
            raw = jnp.dot(block, patches[...], preferred_element_type=jnp.float32)
            value = jnp.exp2(raw * lane_scale[...] * proto_scale)
            weights[pl.ds(pl.multiple_of(tile * BLOCK, BLOCK), BLOCK)] = value
            add_rows(value, jnp.sum(value, axis=1, keepdims=True), tile)
            scales[r, 1, :, pl.ds(pl.multiple_of(tile * BLOCK, BLOCK), BLOCK)] = turned(proto_scale)

        each(width // BLOCK // 2, body)

    def one_pass(it):
        def body(tile):
            at = pl.ds(pl.multiple_of(tile * BLOCK, BLOCK), BLOCK)
            value = weights[at]
            col_mass = jnp.sum(value * row_scale[...], axis=1, keepdims=True)
            col_scale = add_rows(value, col_mass, tile)
            if it == ITERS - 1:
                scales[r, 0, :, at] = turned(col_scale)

        each(width // BLOCK, body)

    def give_rows(it):
        row_out[it] = jnp.sum(acc[...], axis=0, keepdims=True)
        acc[...] = jnp.zeros_like(acc)
        for step in range(1, n_protos):
            row_copy(it, step).start()

    def give_mass(it):
        mass = row_out[it]
        for step in range(1, n_protos):
            row_copy(it, step).wait_recv()
            mass = mass + row_in[it, step]
        mass_out[it] = mass
        for step in range(1, n_rows):
            mass_copy(it, step).start()

    def take_mass(it):
        mass = mass_out[it]
        for step in range(1, n_rows):
            mass_copy(it, step).wait_recv()
            mass = mass + mass_in[it, step]
        row_scale[...] = 1.0 / (masked * mass)

    def next_pass(it):
        take_mass(it - 1)
        one_pass(it)
        if it == ITERS - 1:
            for step in range(1, n_rows):
                scale_copy(step, r).start()
        give_rows(it)

    def settle():
        take_mass(ITERS - 1)
        at = lax.broadcasted_iota(jnp.int32, (rows, lanes), 1)
        row = lax.broadcasted_iota(jnp.int32, (rows, lanes), 0) + r * rows
        found = jnp.where(at == row, jnp.broadcast_to(row_scale[...], (rows, lanes)), 0.0)
        found = jnp.sum(found, axis=1, keepdims=True) * (protos_all * masked)
        out_scale[...] = jnp.broadcast_to(found, out_scale.shape)
        for step in range(1, n_rows):
            scale_copy(step, lax.rem(r + step, n_rows)).wait_recv()

    def make_output(c):
        tile = min(512, span)
        for t in range(span // tile):
            block = full[c, :, t * tile:(t + 1) * tile]
            raw = jnp.dot(chosen[...], block, preferred_element_type=jnp.float32)
            at = pl.ds(pl.multiple_of(lax.rem(c, SPLIT) * span + t * tile, tile), tile)
            value = jnp.exp2(raw * feat_scale[:, :1] * scales[owner(c), 1, :, at])
            value = out_scale[:, :1] * value * scales[owner(c), 0, :, at]
            out_ref[c, :, t * tile:(t + 1) * tile] = value.astype(jnp.bfloat16)

    stages = {
        (0, 2): take_patches,
        (STATS_AT, 3): take_own,
        (1, 0): lambda: make_weights(0),
        (1, 2): lambda: (make_weights(1), give_rows(0)),
        (1, 3): lambda: give_mass(0),
        (2, 3): lambda: next_pass(1),
        (3, 1): lambda: give_mass(1),
        (4, 2): lambda: next_pass(2),
        (4, 3): lambda: give_mass(2),
        (6, 1): settle,
    }
    first = 6

    def hooks(i, place):
        for (at, position), stage in stages.items():
            if position == place:
                when(i == at, stage)

    pace = 4

    def beside(i):
        c = order(ACROSS, i)
        src = other
        when(jnp.logical_or(owner(c) != r, i <= STATS_AT), lambda: block_copy(ACROSS, src, c).wait_recv())
        when(both(early(c), goes_up(c, False)), lambda: block_copy(UP, src, c).start())
        when(both(early(c), goes_down(c, False)), lambda: block_copy(DOWN, src, c).start())

    def ways(d):
        return (
            (DOWN, z + d, goes_down, z + d < nz),
            (UP, z - d, goes_up, z - d >= 0),
        )

    def line(i, k, d):
        for way, ahead, more, there in ways(d):
            src = ahead * 2 + y
            c = order(way, k)

            @pl.when(there)
            def _():
                when(plane(c) != z, lambda: block_copy(ACROSS, src, c).wait_recv())
                when(more(c, True), lambda: block_copy(way, src, c).start())
                when(
                    both(no(early(c)), owner(c) != other), lambda: block_copy(ACROSS, src, c).start()
                )

    def take_far(i, src, c):
        when(
            jnp.logical_or(owner(c) != r, i <= STATS_AT),
            lambda: block_copy(ACROSS, src, c).wait_recv(),
        )

    def early_line(i, d):
        for way, ahead, more, there in ways(d):
            src = ahead * 2 + 1 - y

            @pl.when(there)
            def _():
                for c in EARLY:
                    take_far(i, src, c)
                    when(more(c, False), lambda: block_copy(way, src, c).start())

    def far_line(i, k, d):
        for way, ahead, more, there in ways(d):
            c = order(way, k)
            when(both(there, no(early(c))), lambda: take_far(i, ahead * 2 + 1 - y, c))

    def drain(k):
        across = order(ACROSS, k)
        block_copy(ACROSS, r, across).wait_send()
        for way in (DOWN, UP):
            c = order(way, k)
            for d in range(nz):
                ahead = z + d if way == DOWN else z - d
                more = goes_down(c, True) if way == DOWN else goes_up(c, True)
                there = ahead < nz if way == DOWN else ahead >= 0

                @pl.when(there)
                def _():
                    src = ahead * 2 + y
                    when(more, lambda: block_copy(way, src, c).wait_send())
                    if d > 0:
                        when(
                            jnp.logical_or(no(early(c)), owner(c) == other),
                            lambda: block_copy(ACROSS, src, c).wait_send(),
                        )

    def drain_early():
        for c in EARLY:
            for way in (DOWN, UP):
                for d in range(nz):
                    ahead = z + d if way == DOWN else z - d
                    more = goes_down(c, False) if way == DOWN else goes_up(c, False)
                    there = ahead < nz if way == DOWN else ahead >= 0
                    src = ahead * 2 + 1 - y
                    when(both(there, more), lambda: block_copy(way, src, c).wait_send())

    middle = both(z > 0, z < nz - 1)

    def ready(i):
        last = i - nz + 2
        return jnp.where(middle, 2 * last - chunks, last)

    def done_by(i):
        return jnp.clip(jnp.minimum((i - first + 1) * pace, ready(i)), 0, chunks)

    def nth(k):
        half = chunks // 2
        inner = jnp.where(k % 2 == 0, half - 1 - k // 2, half + k // 2)
        return jnp.where(middle, inner, jnp.where(z == 0, chunks - 1 - k, k))

    def step_of(i, carry):
        for way in (DOWN, UP):
            own_line(way, i + lead(way))
        own_across(i + LEAD_Y)
        when(i < chunks, lambda: beside(i))
        hooks(i, 0)
        for d in range(1, nz):
            k = i - (d - 1)
            when(both(k >= 0, k < chunks), lambda: line(i, k, d))
            if d < nz - 1:
                hooks(i, d)
        for d in range(1, nz):
            when(i == EARLY_AT + d, lambda: early_line(i, d))
        last = i - (nz - 1)

        @pl.when(last >= 0)
        def _():
            for d in range(1, nz):
                far_line(i, last, d)

        hooks(i, 3)

        def output(k, carry):
            make_output(nth(k))
            return carry

        lax.fori_loop(done_by(i - 1), done_by(i), output, 0)
        when(last >= LAG, lambda: drain(last - LAG))
        return carry

    relay()
    steps = chunks + nz - 1
    lax.fori_loop(0, steps, step_of, 0)

    for step in range(1, n_rows):
        pick_copy(step).wait_send()
        scale_copy(step, r).wait_send()
    for step in range(1, nz):
        for c in range(2 * SPLIT):
            direct_copy(step, c).wait_send()
    for step in range(1, n_protos):
        patch_copy(step, p).wait_send()
    for it in range(ITERS):
        for step in range(1, n_rows):
            mass_copy(it, step).wait_send()
        for step in range(1, n_protos):
            row_copy(it, step).wait_send()

    def rest(i, carry):
        drain(i)
        return carry

    lax.fori_loop(chunks - LAG, chunks, rest, 0)
    drain_early()


def finish(blocks_ref, out_ref, out_sem):
    count, rows, span = blocks_ref.shape
    copies = [
        pltpu.make_async_copy(
            blocks_ref.at[c], out_ref.at[:, c * span:(c + 1) * span], out_sem.at[c]
        )
        for c in range(count)
    ]
    for copy in copies:
        copy.start()
    for copy in copies:
        copy.wait()


def with_kernel(n_rows, n_protos, features, prototypes, masked_index):
    rows = masked_index.shape[0]
    dim, total = prototypes.shape[1], prototypes.shape[0]
    fdim, patches = features.shape[1], features.shape[0]
    width = total // n_rows
    chunks = n_rows * SPLIT
    span = total // chunks
    lanes = rows * n_rows
    depth = fdim * n_protos
    masked = float(lanes)
    protos_all = float(total * n_protos)
    f32, bf16, dma = jnp.float32, jnp.bfloat16, pltpu.SemaphoreType.DMA
    vmem = pl.BlockSpec(memory_space=pltpu.VMEM)
    anywhere = pl.BlockSpec(memory_space=pl.ANY)
    blocks = pl.pallas_call(
        functools.partial(kernel, n_rows, n_protos, masked, protos_all),
        out_shape=jax.ShapeDtypeStruct((chunks, rows, span), bf16),
        in_specs=[pl.BlockSpec(memory_space=pltpu.HBM)] * 3,
        out_specs=vmem,
        scratch_shapes=[
            pltpu.VMEM((fdim, patches), bf16),
            pltpu.VMEM((1, rows), jnp.int32),
            pltpu.VMEM((patches, 2 * BLOCK), bf16),
            pltpu.VMEM((n_rows, fdim, 2 * BLOCK), bf16),
            pltpu.VMEM((depth, lanes), bf16),
            pltpu.VMEM((2 * rows, depth), bf16),
            pltpu.VMEM((rows, depth), bf16),
            pltpu.VMEM((1, lanes), f32),
            pltpu.VMEM((rows, BLOCK), f32),
            pltpu.VMEM((chunks, dim * n_rows, span), bf16),
            pltpu.VMEM((width, lanes), f32),
            pltpu.VMEM((8, lanes), f32),
            pltpu.VMEM((ITERS, 1, lanes), f32),
            pltpu.VMEM((ITERS, n_protos, 1, lanes), f32),
            pltpu.VMEM((ITERS, 1, lanes), f32),
            pltpu.VMEM((ITERS, n_rows, 1, lanes), f32),
            pltpu.VMEM((1, lanes), f32),
            pltpu.VMEM((rows, BLOCK), f32),
            pltpu.VMEM((n_rows, 2, 1, width), f32),
            dma((2,)),
            dma((chunks,)),
            dma((n_rows,)),
            dma((n_rows,)),
            dma((n_protos,)),
            dma((n_protos,)),
            dma((3, n_rows, chunks)),
            dma((n_rows, chunks)),
            dma((n_rows // 2, 2 * SPLIT)),
            dma((ITERS, n_protos)),
            dma((ITERS, n_protos)),
            dma((ITERS, n_rows)),
            dma((ITERS, n_rows)),
            dma((n_rows,)),
            dma((n_rows,)),
        ],
        compiler_params=pltpu.CompilerParams(
            collective_id=0, has_side_effects=True, vmem_limit_bytes=46 * 1024 * 1024
        ),
    )(features.T, prototypes.T, masked_index[None, :])
    return pl.pallas_call(
        finish,
        out_shape=jax.ShapeDtypeStruct((rows, total), bf16),
        in_specs=[vmem],
        out_specs=anywhere,
        scratch_shapes=[dma((chunks,))],
        compiler_params=pltpu.CompilerParams(vmem_limit_bytes=4 * 1024 * 1024),
    )(blocks)


def with_collectives(features, prototypes, masked_index):
    total_protos = float(prototypes.shape[0] * lax.axis_size("protos"))
    chosen = jnp.take(features, masked_index, axis=0)
    patches = lax.all_gather(chosen, "protos", axis=1, tiled=True)
    feat_scale = lax.rsqrt(jnp.sum(jnp.square(patches.astype(jnp.float32)), axis=1) + EPS)
    full = lax.all_gather(prototypes, "rows", axis=1, tiled=True)
    proto_sq = jnp.sum(jnp.square(full.astype(jnp.float32)), axis=1)
    raw = lax.dot_general(
        patches, full, (((1,), (1,)), ((), ())), preferred_element_type=jnp.float32
    )
    proto_scale = lax.rsqrt(proto_sq + EPS)
    weights = jnp.exp(raw * feat_scale[:, None] * proto_scale[None, :] / TEMP)
    total_rows = masked_index.shape[0] * lax.axis_size("rows")
    row_scale = jnp.ones((patches.shape[0],), jnp.float32)
    for step in range(ITERS):
        col_part = jnp.dot(row_scale, weights, precision=lax.Precision.HIGHEST)
        col_scale = 1.0 / (total_protos * lax.psum(col_part, "rows"))
        row_part = jnp.dot(weights, col_scale, precision=lax.Precision.HIGHEST)
        row_scale = 1.0 / (total_rows * lax.psum(row_part, "protos"))
    factor = total_protos * float(total_rows)
    return (factor * row_scale[:, None] * weights * col_scale[None, :]).astype(jnp.bfloat16)


def solution(mesh):
    n_rows, n_protos = mesh.shape["rows"], mesh.shape["protos"]
    in_specs = (P("rows", "protos"), P("protos", "rows"), P("rows"))
    out_specs = P("rows", "protos")

    def on_device(features, prototypes, masked_index):
        fits = (
            n_rows % 2 == 0
            and n_rows == 8
            and n_protos > 1
            and prototypes.shape[1] % 16 == 0
            and features.shape[1] % 16 == 0
            and features.shape[1] * n_protos == prototypes.shape[1] * n_rows
            and 2 * masked_index.shape[0] == 3 * BLOCK
            and prototypes.shape[0] % (n_rows * SPLIT * 512) == 0
        )
        if fits:
            return with_kernel(n_rows, n_protos, features, prototypes, masked_index)
        return with_collectives(features, prototypes, masked_index)

    return jax.shard_map(
        on_device, mesh=mesh, in_specs=in_specs, out_specs=out_specs, check_vma=False
    )
```

```python
import functools

import jax
import jax.numpy as jnp
from jax import lax
from jax.experimental import pallas as pl
from jax.experimental.pallas import tpu as pltpu
from jax.sharding import PartitionSpec as P

ITERS = 3


TEMP = 0.07
EPS = 1e-06
LOG2E = 1.4426950408889634
UP, DOWN, ACROSS = 0, 1, 2
LEAD_Z = (8, 3, 6, 0)
LEAD_Y = 8
FIRST_Z = 1
FIRST_Y = 1
SPLIT = 1
EARLY = (4,)
EARLY_AT = 3
LAG = 2
STATS_AT = 0
BLOCK = 128


def kernel(
    n_rows, n_protos, masked, protos_all,
    feat_ref, proto_ref, index_ref, out_ref,
    feat_in, index, onehot, picks, patches, pair, chosen, lane_scale, feat_scale, full, weights,
    acc, row_out, row_in, mass_out, mass_in, row_scale, out_scale, scales,
    line_sem, in_sem, own_sem, pick_send, pick_recv, patch_send, patch_recv, send, recv, direct_send,
    row_send, row_recv, mass_send, mass_recv, scale_send, scale_recv,
):
    r, p = lax.axis_index("rows"), lax.axis_index("protos")
    z, y = r // 2, lax.rem(r, 2)
    nz = n_rows // 2
    other = z * 2 + 1 - y
    dim, total = proto_ref.shape
    width = total // n_rows
    chunks = n_rows * SPLIT
    span = total // chunks
    rows = index_ref.shape[1]
    fdim = feat_ref.shape[0]
    lanes = rows * n_rows
    odd = y == 1
    both = jnp.logical_and
    no = jnp.logical_not
    mesh_id = pl.DeviceIdType.MESH

    def where(src, c):
        return full.at[c, pl.ds(pl.multiple_of(src * dim, dim), dim)]

    def own_copy(c):
        return pltpu.make_async_copy(
            proto_ref.at[:, pl.ds(pl.multiple_of(c * span, span), span)], where(r, c), own_sem.at[c]
        )

    def early(c):
        hit = c == EARLY[0]
        for e in EARLY[1:]:
            hit = jnp.logical_or(hit, c == e)
        return hit

    def owner(c):
        return c // SPLIT

    def plane(c):
        return c // (2 * SPLIT)

    def remote(src, dst, send_sem, recv_sem, **device):
        return pltpu.make_async_remote_copy(
            src_ref=src, dst_ref=dst, send_sem=send_sem, recv_sem=recv_sem,
            device_id=device, device_id_type=mesh_id,
        )

    def block_copy(way, src, c):
        target = {UP: r + 2, DOWN: r - 2, ACROSS: other}[way]
        return remote(where(src, c), where(src, c), send.at[way, src, c], recv.at[src, c], rows=target)

    def when(condition, action):
        @pl.when(condition)
        def _():
            action()

    def each(count, body):
        def step(i, carry):
            body(i)
            return carry

        lax.fori_loop(0, count, step, 0)

    def goes_up(c, on_line):
        return both(z < nz - 1, plane(c) != z + 1 if on_line else owner(c) != r + 2)

    def goes_down(c, on_line):
        return both(z > 0, plane(c) != z - 1 if on_line else owner(c) != r - 2)

    def direct_copy(step, c):
        target = lax.rem(r + 2 * step, n_rows)
        chunk = target // 2 * (2 * SPLIT) + c
        return remote(
            where(r, chunk), where(r, chunk), direct_send.at[step, c], recv.at[r, chunk], rows=target
        )

    def pick_copy(step):
        return remote(
            picks.at[y, z], picks.at[y, z], pick_send.at[step], pick_recv.at[z],
            rows=lax.rem(r + 2 * step, n_rows),
        )

    def picks_across(column):
        return remote(picks.at[column], picks.at[column], pick_send.at[0], pick_recv.at[nz], rows=other)

    def patch_copy(step, src):
        part = patches.at[pl.ds(pl.multiple_of(src * fdim, fdim), fdim)]
        return remote(
            part, part, patch_send.at[step], patch_recv.at[src], protos=lax.rem(p + step, n_protos)
        )

    def row_copy(it, step):
        return remote(
            row_out.at[it], row_in.at[it, step], row_send.at[it, step], row_recv.at[it, step],
            protos=lax.rem(p + step, n_protos),
        )

    def mass_copy(it, step):
        return remote(
            mass_out.at[it], mass_in.at[it, step], mass_send.at[it, step], mass_recv.at[it, step],
            rows=lax.rem(r + step, n_rows),
        )

    def scale_copy(step, src):
        return remote(
            scales.at[src], scales.at[src], scale_send.at[step], scale_recv.at[src],
            rows=lax.rem(r + step, n_rows),
        )

    feat_load = pltpu.make_async_copy(feat_ref, feat_in, in_sem.at[0])
    index_load = pltpu.make_async_copy(index_ref, index, in_sem.at[1])
    feat_load.start()
    index_load.start()
    each(chunks, lambda c: own_copy(c).start())

    barrier = pltpu.get_barrier_semaphore()

    def greet(semaphore, **device):
        pl.semaphore_signal(semaphore, inc=1, device_id=device, device_id_type=mesh_id)

    greet(barrier, rows=other)
    when(z > 0, lambda: greet(barrier, rows=r - 2))
    when(z < nz - 1, lambda: greet(barrier, rows=r + 2))
    for step in range(1, n_protos):
        greet(barrier, protos=lax.rem(p + step, n_protos))

    onehot[...] = jnp.zeros_like(onehot)
    index_load.wait()
    hits = lax.broadcasted_iota(jnp.int32, (onehot.shape[0], rows), 0) == index[...]
    onehot[:, :rows] = hits.astype(jnp.float32).astype(jnp.bfloat16)
    feat_load.wait()
    picked = jnp.dot(feat_in[...], onehot[...], preferred_element_type=jnp.float32)
    picked = jnp.where(odd, pltpu.roll(picked, 2 * BLOCK - rows, 1), picked)
    picks[y, z] = picked.astype(jnp.bfloat16)
    acc[...] = jnp.zeros_like(acc)
    each(chunks, lambda c: own_copy(c).wait())

    def order(way, k):
        if way == ACROSS:
            swapped = jnp.where(both(k >= EARLY_AT, k <= EARLY_AT + 1), 2 * EARLY_AT + 1 - k, k)
            return jnp.where(z < nz // 2, chunks - 1 - k, swapped)
        return k if way == UP else chunks - 1 - k

    def lead(way):
        behind = z if way == UP else nz - 1 - z
        count = LEAD_Z[nz - 1]
        for at in range(nz - 1):
            count = jnp.where(behind == at, LEAD_Z[at], count)
        return count

    def own_line(way, k):
        c = order(way, k)
        more = (goes_up if way == UP else goes_down)(c, True)
        when(both(k < chunks, more), lambda: block_copy(way, r, c).start())

    def own_across(k):
        c = order(ACROSS, k)
        when(both(k < chunks, owner(c) != other), lambda: block_copy(ACROSS, r, c).start())

    def hear(sem, behind, ahead_there, ahead):
        when(behind, lambda: pl.semaphore_wait(sem, 1))
        when(ahead_there, lambda: greet(sem, rows=ahead))

    def hear_up():
        hear(line_sem.at[UP], z > 0, z < nz - 1, r + 2)

    def hear_down():
        hear(line_sem.at[DOWN], z < nz - 1, z > 0, r - 2)

    met = n_protos - 1 + 1 + jnp.where(z > 0, 1, 0) + jnp.where(z < nz - 1, 1, 0)
    pl.semaphore_wait(barrier, met)
    for way in (DOWN, UP):
        for k in range(FIRST_Z):
            own_line(way, k)
    for j in range(SPLIT):
        block_copy(ACROSS, r, other * SPLIT + j).start()
    for k in range(FIRST_Y):
        own_across(k)

    @pl.when(z < nz // 2)
    def _():
        hear_up()
        hear_down()

    @pl.when(z >= nz // 2)
    def _():
        hear_down()
        hear_up()

    for step in range(1, nz):
        pick_copy(step).start()
    for apart in range(1, nz):
        for side in (1, -1):
            there = both(z + side * apart >= 0, z + side * apart < nz)
            for c in range(2 * SPLIT):
                when(there, lambda: direct_copy(lax.rem(nz + side * apart, nz), c).start())
    for way in (DOWN, UP):
        each(lead(way) - FIRST_Z, lambda k: own_line(way, k + FIRST_Z))

    for step in range(1, nz):
        src = lax.rem(z + step, nz)
        remote(
            picks.at[y, src], picks.at[y, src], pick_send.at[0], pick_recv.at[src], rows=other
        ).wait_recv()
    picks_across(y).start()
    each(LEAD_Y - FIRST_Y, lambda k: own_across(k + FIRST_Y))
    picks_across(1 - y).wait_recv()
    mine = pl.ds(pl.multiple_of(p * fdim, fdim), fdim)
    for j in range(nz):
        at = 3 * BLOCK * j
        patches[mine, at:at + BLOCK] = picks[0, j, :, :BLOCK]
        patches[mine, at + BLOCK:at + 2 * BLOCK] = (
            picks[0, j, :, BLOCK:].astype(jnp.float32) + picks[1, j, :, :BLOCK].astype(jnp.float32)
        ).astype(jnp.bfloat16)
        patches[mine, at + 2 * BLOCK:at + 3 * BLOCK] = picks[1, j, :, BLOCK:]
    for step in range(1, n_protos):
        patch_copy(step, p).start()

    def relay():
        for apart in range(1, nz):
            for side in (1, -1):
                ahead = z + side * apart
                src = ahead * 2 + y

                @pl.when(both(ahead >= 0, ahead < nz))
                def _():
                    for j in range(SPLIT):
                        block_copy(ACROSS, src, other * SPLIT + j).wait_recv()
                        block_copy(ACROSS, src, other * SPLIT + j).start()
                    for j in range(SPLIT):
                        block_copy(ACROSS, src, r * SPLIT + j).wait_recv()

    def take_patches():
        for step in range(1, n_protos):
            patch_copy(step, lax.rem(p + step, n_protos)).wait_recv()
        pair[...] = patches[:, pl.ds(pl.multiple_of(z * (2 * rows), 2 * rows), 2 * rows)].T
        chosen[...] = pair[pl.ds(pl.multiple_of(y * rows, rows), rows), :]
        wide = chosen[...].astype(jnp.float32)
        scale = lax.rsqrt(jnp.sum(wide * wide, axis=1, keepdims=True) + EPS)
        feat_scale[...] = jnp.broadcast_to(scale * (LOG2E / TEMP), feat_scale.shape)
        for t in range(lanes // BLOCK):
            wide = patches[:, t * BLOCK:(t + 1) * BLOCK].astype(jnp.float32)
            scale = lax.rsqrt(jnp.sum(wide * wide, axis=0, keepdims=True) + EPS)
            lane_scale[:, t * BLOCK:(t + 1) * BLOCK] = scale * (LOG2E / TEMP)

    def take_own():
        for step in range(nz):
            src = lax.rem(other + 2 * step, n_rows)
            apart = jnp.abs(src // 2 - z)
            for j in range(SPLIT):
                c = r * SPLIT + j
                k = jnp.where(src // 2 > z, order(DOWN, c), c)
                at = jnp.where(early(c), EARLY_AT + apart, k + nz - 1)
                at = jnp.where(apart == 0, order(ACROSS, c), at)
                when(at > STATS_AT, lambda: block_copy(ACROSS, src, c).wait_recv())

    def turned(column):
        return jnp.broadcast_to(column, (BLOCK, BLOCK)).T[:1]

    def add_rows(value, col_mass, tile):
        col_scale = 1.0 / (protos_all * col_mass)
        scaled = (value * col_scale).reshape(BLOCK // 8, 8, lanes)
        acc[...] += jnp.sum(scaled, axis=0)
        return col_scale

    def make_weights(half):
        def body(i):
            tile = half * (width // BLOCK // 2) + i
            per = span // BLOCK
            within = pl.ds(pl.multiple_of(lax.rem(tile, per) * BLOCK, BLOCK), BLOCK)
            block = full[r * SPLIT + tile // per, :, within].T
            wide = block.astype(jnp.float32)
            proto_scale = lax.rsqrt(jnp.sum(wide * wide, axis=1, keepdims=True) + EPS)
            raw = jnp.dot(block, patches[...], preferred_element_type=jnp.float32)
            value = jnp.exp2(raw * lane_scale[...] * proto_scale)
            weights[pl.ds(pl.multiple_of(tile * BLOCK, BLOCK), BLOCK)] = value
            add_rows(value, jnp.sum(value, axis=1, keepdims=True), tile)
            scales[r, 1, :, pl.ds(pl.multiple_of(tile * BLOCK, BLOCK), BLOCK)] = turned(proto_scale)

        each(width // BLOCK // 2, body)

    def one_pass(it):
        def body(tile):
            at = pl.ds(pl.multiple_of(tile * BLOCK, BLOCK), BLOCK)
            value = weights[at]
            col_mass = jnp.sum(value * row_scale[...], axis=1, keepdims=True)
            col_scale = add_rows(value, col_mass, tile)
            if it == ITERS - 1:
                scales[r, 0, :, at] = turned(col_scale)

        each(width // BLOCK, body)

    def give_rows(it):
        row_out[it] = jnp.sum(acc[...], axis=0, keepdims=True)
        acc[...] = jnp.zeros_like(acc)
        for step in range(1, n_protos):
            row_copy(it, step).start()

    def give_mass(it):
        mass = row_out[it]
        for step in range(1, n_protos):
            row_copy(it, step).wait_recv()
            mass = mass + row_in[it, step]
        mass_out[it] = mass
        for step in range(1, n_rows):
            mass_copy(it, step).start()

    def take_mass(it):
        mass = mass_out[it]
        for step in range(1, n_rows):
            mass_copy(it, step).wait_recv()
            mass = mass + mass_in[it, step]
        row_scale[...] = 1.0 / (masked * mass)

    def next_pass(it):
        take_mass(it - 1)
        one_pass(it)
        if it == ITERS - 1:
            for step in range(1, n_rows):
                scale_copy(step, r).start()
        give_rows(it)

    def settle():
        take_mass(ITERS - 1)
        at = lax.broadcasted_iota(jnp.int32, (rows, lanes), 1)
        row = lax.broadcasted_iota(jnp.int32, (rows, lanes), 0) + r * rows
        found = jnp.where(at == row, jnp.broadcast_to(row_scale[...], (rows, lanes)), 0.0)
        found = jnp.sum(found, axis=1, keepdims=True) * (protos_all * masked)
        out_scale[...] = jnp.broadcast_to(found, out_scale.shape)
        for step in range(1, n_rows):
            scale_copy(step, lax.rem(r + step, n_rows)).wait_recv()

    def make_output(c):
        tile = min(512, span)
        for t in range(span // tile):
            block = full[c, :, t * tile:(t + 1) * tile]
            raw = jnp.dot(chosen[...], block, preferred_element_type=jnp.float32)
            at = pl.ds(pl.multiple_of(lax.rem(c, SPLIT) * span + t * tile, tile), tile)
            value = jnp.exp2(raw * feat_scale[:, :1] * scales[owner(c), 1, :, at])
            value = out_scale[:, :1] * value * scales[owner(c), 0, :, at]
            out_ref[c, :, t * tile:(t + 1) * tile] = value.astype(jnp.bfloat16)

    stages = {
        (0, 2): take_patches,
        (STATS_AT, 3): take_own,
        (1, 0): lambda: make_weights(0),
        (1, 2): lambda: (make_weights(1), give_rows(0)),
        (1, 3): lambda: give_mass(0),
        (2, 3): lambda: next_pass(1),
        (3, 1): lambda: give_mass(1),
        (4, 2): lambda: next_pass(2),
        (4, 3): lambda: give_mass(2),
        (6, 1): settle,
    }
    first = 6

    def hooks(i, place):
        for (at, position), stage in stages.items():
            if position == place:
                when(i == at, stage)

    pace = 4

    def beside(i):
        c = order(ACROSS, i)
        src = other
        when(jnp.logical_or(owner(c) != r, i <= STATS_AT), lambda: block_copy(ACROSS, src, c).wait_recv())
        when(both(early(c), goes_up(c, False)), lambda: block_copy(UP, src, c).start())
        when(both(early(c), goes_down(c, False)), lambda: block_copy(DOWN, src, c).start())

    def ways(d):
        return (
            (DOWN, z + d, goes_down, z + d < nz),
            (UP, z - d, goes_up, z - d >= 0),
        )

    def line(i, k, d):
        for way, ahead, more, there in ways(d):
            src = ahead * 2 + y
            c = order(way, k)

            @pl.when(there)
            def _():
                when(plane(c) != z, lambda: block_copy(ACROSS, src, c).wait_recv())
                when(more(c, True), lambda: block_copy(way, src, c).start())
                when(
                    both(no(early(c)), owner(c) != other), lambda: block_copy(ACROSS, src, c).start()
                )

    def take_far(i, src, c):
        when(
            jnp.logical_or(owner(c) != r, i <= STATS_AT),
            lambda: block_copy(ACROSS, src, c).wait_recv(),
        )

    def early_line(i, d):
        for way, ahead, more, there in ways(d):
            src = ahead * 2 + 1 - y

            @pl.when(there)
            def _():
                for c in EARLY:
                    take_far(i, src, c)
                    when(more(c, False), lambda: block_copy(way, src, c).start())

    def far_line(i, k, d):
        for way, ahead, more, there in ways(d):
            c = order(way, k)
            when(both(there, no(early(c))), lambda: take_far(i, ahead * 2 + 1 - y, c))

    def drain(k):
        across = order(ACROSS, k)
        block_copy(ACROSS, r, across).wait_send()
        for way in (DOWN, UP):
            c = order(way, k)
            for d in range(nz):
                ahead = z + d if way == DOWN else z - d
                more = goes_down(c, True) if way == DOWN else goes_up(c, True)
                there = ahead < nz if way == DOWN else ahead >= 0

                @pl.when(there)
                def _():
                    src = ahead * 2 + y
                    when(more, lambda: block_copy(way, src, c).wait_send())
                    if d > 0:
                        when(
                            jnp.logical_or(no(early(c)), owner(c) == other),
                            lambda: block_copy(ACROSS, src, c).wait_send(),
                        )

    def drain_early():
        for c in EARLY:
            for way in (DOWN, UP):
                for d in range(nz):
                    ahead = z + d if way == DOWN else z - d
                    more = goes_down(c, False) if way == DOWN else goes_up(c, False)
                    there = ahead < nz if way == DOWN else ahead >= 0
                    src = ahead * 2 + 1 - y
                    when(both(there, more), lambda: block_copy(way, src, c).wait_send())

    middle = both(z > 0, z < nz - 1)

    def ready(i):
        last = i - nz + 2
        return jnp.where(middle, 2 * last - chunks, last)

    def done_by(i):
        return jnp.clip(jnp.minimum((i - first + 1) * pace, ready(i)), 0, chunks)

    def nth(k):
        half = chunks // 2
        inner = jnp.where(k % 2 == 0, half - 1 - k // 2, half + k // 2)
        return jnp.where(middle, inner, jnp.where(z == 0, chunks - 1 - k, k))

    def step_of(i, carry):
        for way in (DOWN, UP):
            own_line(way, i + lead(way))
        own_across(i + LEAD_Y)
        when(i < chunks, lambda: beside(i))
        hooks(i, 0)
        for d in range(1, nz):
            k = i - (d - 1)
            when(both(k >= 0, k < chunks), lambda: line(i, k, d))
            if d < nz - 1:
                hooks(i, d)
        for d in range(1, nz):
            when(i == EARLY_AT + d, lambda: early_line(i, d))
        last = i - (nz - 1)

        @pl.when(last >= 0)
        def _():
            for d in range(1, nz):
                far_line(i, last, d)

        hooks(i, 3)

        def output(k, carry):
            make_output(nth(k))
            return carry

        lax.fori_loop(done_by(i - 1), done_by(i), output, 0)
        when(last >= LAG, lambda: drain(last - LAG))
        return carry

    relay()
    steps = chunks + nz - 1
    lax.fori_loop(0, steps, step_of, 0)

    picks_across(y).wait_send()
    for step in range(1, nz):
        pick_copy(step).wait_send()
    for step in range(1, n_rows):
        scale_copy(step, r).wait_send()
    for step in range(1, nz):
        for c in range(2 * SPLIT):
            direct_copy(step, c).wait_send()
    for step in range(1, n_protos):
        patch_copy(step, p).wait_send()
    for it in range(ITERS):
        for step in range(1, n_rows):
            mass_copy(it, step).wait_send()
        for step in range(1, n_protos):
            row_copy(it, step).wait_send()

    def rest(i, carry):
        drain(i)
        return carry

    lax.fori_loop(chunks - LAG, chunks, rest, 0)
    drain_early()


def finish(blocks_ref, out_ref, out_sem):
    count, rows, span = blocks_ref.shape
    copies = [
        pltpu.make_async_copy(
            blocks_ref.at[c], out_ref.at[:, c * span:(c + 1) * span], out_sem.at[c]
        )
        for c in range(count)
    ]
    for copy in copies:
        copy.start()
    for copy in copies:
        copy.wait()


def with_kernel(n_rows, n_protos, features, prototypes, masked_index):
    rows = masked_index.shape[0]
    dim, total = prototypes.shape[1], prototypes.shape[0]
    fdim, patches = features.shape[1], features.shape[0]
    width = total // n_rows
    chunks = n_rows * SPLIT
    span = total // chunks
    lanes = rows * n_rows
    depth = fdim * n_protos
    masked = float(lanes)
    protos_all = float(total * n_protos)
    f32, bf16, dma = jnp.float32, jnp.bfloat16, pltpu.SemaphoreType.DMA
    vmem = pl.BlockSpec(memory_space=pltpu.VMEM)
    anywhere = pl.BlockSpec(memory_space=pl.ANY)
    blocks = pl.pallas_call(
        functools.partial(kernel, n_rows, n_protos, masked, protos_all),
        out_shape=jax.ShapeDtypeStruct((chunks, rows, span), bf16),
        in_specs=[pl.BlockSpec(memory_space=pltpu.HBM)] * 3,
        out_specs=vmem,
        scratch_shapes=[
            pltpu.VMEM((fdim, patches), bf16),
            pltpu.VMEM((1, rows), jnp.int32),
            pltpu.VMEM((patches, 2 * BLOCK), bf16),
            pltpu.VMEM((2, n_rows // 2, fdim, 2 * BLOCK), bf16),
            pltpu.VMEM((depth, lanes), bf16),
            pltpu.VMEM((2 * rows, depth), bf16),
            pltpu.VMEM((rows, depth), bf16),
            pltpu.VMEM((1, lanes), f32),
            pltpu.VMEM((rows, BLOCK), f32),
            pltpu.VMEM((chunks, dim * n_rows, span), bf16),
            pltpu.VMEM((width, lanes), f32),
            pltpu.VMEM((8, lanes), f32),
            pltpu.VMEM((ITERS, 1, lanes), f32),
            pltpu.VMEM((ITERS, n_protos, 1, lanes), f32),
            pltpu.VMEM((ITERS, 1, lanes), f32),
            pltpu.VMEM((ITERS, n_rows, 1, lanes), f32),
            pltpu.VMEM((1, lanes), f32),
            pltpu.VMEM((rows, BLOCK), f32),
            pltpu.VMEM((n_rows, 2, 1, width), f32),
            pltpu.SemaphoreType.REGULAR((2,)),
            dma((2,)),
            dma((chunks,)),
            dma((n_rows,)),
            dma((n_rows,)),
            dma((n_protos,)),
            dma((n_protos,)),
            dma((3, n_rows, chunks)),
            dma((n_rows, chunks)),
            dma((n_rows // 2, 2 * SPLIT)),
            dma((ITERS, n_protos)),
            dma((ITERS, n_protos)),
            dma((ITERS, n_rows)),
            dma((ITERS, n_rows)),
            dma((n_rows,)),
            dma((n_rows,)),
        ],
        compiler_params=pltpu.CompilerParams(
            collective_id=0, has_side_effects=True, vmem_limit_bytes=46 * 1024 * 1024
        ),
    )(*(pltpu.with_memory_space_constraint(x, pltpu.HBM) for x in (features.T, prototypes.T, masked_index[None, :])))
    return pl.pallas_call(
        finish,
        out_shape=jax.ShapeDtypeStruct((rows, total), bf16),
        in_specs=[vmem],
        out_specs=anywhere,
        scratch_shapes=[dma((chunks,))],
        compiler_params=pltpu.CompilerParams(vmem_limit_bytes=4 * 1024 * 1024),
    )(blocks)


def with_collectives(features, prototypes, masked_index):
    total_protos = float(prototypes.shape[0] * lax.axis_size("protos"))
    chosen = jnp.take(features, masked_index, axis=0)
    patches = lax.all_gather(chosen, "protos", axis=1, tiled=True)
    feat_scale = lax.rsqrt(jnp.sum(jnp.square(patches.astype(jnp.float32)), axis=1) + EPS)
    full = lax.all_gather(prototypes, "rows", axis=1, tiled=True)
    proto_sq = jnp.sum(jnp.square(full.astype(jnp.float32)), axis=1)
    raw = lax.dot_general(
        patches, full, (((1,), (1,)), ((), ())), preferred_element_type=jnp.float32
    )
    proto_scale = lax.rsqrt(proto_sq + EPS)
    weights = jnp.exp(raw * feat_scale[:, None] * proto_scale[None, :] / TEMP)
    total_rows = masked_index.shape[0] * lax.axis_size("rows")
    row_scale = jnp.ones((patches.shape[0],), jnp.float32)
    for step in range(ITERS):
        col_part = jnp.dot(row_scale, weights, precision=lax.Precision.HIGHEST)
        col_scale = 1.0 / (total_protos * lax.psum(col_part, "rows"))
        row_part = jnp.dot(weights, col_scale, precision=lax.Precision.HIGHEST)
        row_scale = 1.0 / (total_rows * lax.psum(row_part, "protos"))
    factor = total_protos * float(total_rows)
    return (factor * row_scale[:, None] * weights * col_scale[None, :]).astype(jnp.bfloat16)


def solution(mesh):
    n_rows, n_protos = mesh.shape["rows"], mesh.shape["protos"]
    in_specs = (P("rows", "protos"), P("protos", "rows"), P("rows"))
    out_specs = P("rows", "protos")

    def on_device(features, prototypes, masked_index):
        fits = (
            n_rows % 2 == 0
            and n_rows == 8
            and n_protos > 1
            and prototypes.shape[1] % 16 == 0
            and features.shape[1] % 16 == 0
            and features.shape[1] * n_protos == prototypes.shape[1] * n_rows
            and 2 * masked_index.shape[0] == 3 * BLOCK
            and prototypes.shape[0] % (n_rows * SPLIT * 512) == 0
        )
        if fits:
            return with_kernel(n_rows, n_protos, features, prototypes, masked_index)
        return with_collectives(features, prototypes, masked_index)

    return jax.shard_map(
        on_device, mesh=mesh, in_specs=in_specs, out_specs=out_specs, check_vma=False
    )
```

```python
import functools

import jax
import jax.numpy as jnp
from jax import lax
from jax.experimental import pallas as pl
from jax.experimental.pallas import tpu as pltpu
from jax.sharding import PartitionSpec as P

ITERS = 3


TEMP = 0.07
EPS = 1e-06
LOG2E = 1.4426950408889634
UP, DOWN, ACROSS = 0, 1, 2
LEAD_Z = (8, 3, 6, 0)
LEAD_Y = 8
FIRST_Z = 1
FIRST_Y = 2
SPLIT = 1
EARLY = (4,)
EARLY_AT = 3
LAG = 2
STATS_AT = 1
STAGES = (3, 3, 6, 7, 8, 9, 11, 15, 17, 22, 24, 28)
BLOCK = 128
TILE = 256
PARTS = 2


def kernel(
    n_rows, n_protos, masked, protos_all,
    feat_ref, proto_ref, index_ref, out_ref,
    feat_in, index, onehot, picks, pairs, patches, pair, chosen, lane_scale, feat_scale, full, weights,
    acc, row_out, row_in, mass_out, mass_in, row_scale, out_scale, scales,
    line_sem, in_sem, own_sem, pick_send, pick_recv, patch_send, patch_recv, send, recv, direct_send,
    row_send, row_recv, mass_send, mass_recv, scale_send, scale_recv,
):
    r, p = lax.axis_index("rows"), lax.axis_index("protos")
    z, y = r // 2, lax.rem(r, 2)
    nz = n_rows // 2
    other = z * 2 + 1 - y
    dim, total = proto_ref.shape
    width = total // n_rows
    chunks = n_rows * SPLIT
    span = total // chunks
    rows = index_ref.shape[1]
    fdim = feat_ref.shape[0]
    lanes = rows * n_rows
    odd = y == 1
    both = jnp.logical_and
    no = jnp.logical_not
    mesh_id = pl.DeviceIdType.MESH

    def where(src, c):
        return full.at[c, pl.ds(pl.multiple_of(src * dim, dim), dim)]

    def own_copy(c):
        return pltpu.make_async_copy(
            proto_ref.at[:, pl.ds(pl.multiple_of(c * span, span), span)], where(r, c), own_sem.at[c]
        )

    def early(c):
        hit = c == EARLY[0]
        for e in EARLY[1:]:
            hit = jnp.logical_or(hit, c == e)
        return hit

    def owner(c):
        return c // SPLIT

    def plane(c):
        return c // (2 * SPLIT)

    def remote(src, dst, send_sem, recv_sem, **device):
        return pltpu.make_async_remote_copy(
            src_ref=src, dst_ref=dst, send_sem=send_sem, recv_sem=recv_sem,
            device_id=device, device_id_type=mesh_id,
        )

    def block_copy(way, src, c):
        target = {UP: r + 2, DOWN: r - 2, ACROSS: other}[way]
        return remote(where(src, c), where(src, c), send.at[way, src, c], recv.at[src, c], rows=target)

    def when(condition, action):
        @pl.when(condition)
        def _():
            action()

    def each(count, body):
        def step(i, carry):
            body(i)
            return carry

        lax.fori_loop(0, count, step, 0)

    def goes_up(c, on_line):
        return both(z < nz - 1, plane(c) != z + 1 if on_line else owner(c) != r + 2)

    def goes_down(c, on_line):
        return both(z > 0, plane(c) != z - 1 if on_line else owner(c) != r - 2)

    def direct_copy(step, c):
        target = lax.rem(r + 2 * step, n_rows)
        chunk = target // 2 * (2 * SPLIT) + c
        return remote(
            where(r, chunk), where(r, chunk), direct_send.at[step, c], recv.at[r, chunk], rows=target
        )

    def pick_across():
        return remote(picks.at[0], picks.at[1], pick_send.at[0], pick_recv.at[nz], rows=other)

    def pick_copy(step, src):
        return remote(
            pairs.at[src], pairs.at[src], pick_send.at[step], pick_recv.at[src],
            rows=lax.rem(r + 2 * step, n_rows),
        )

    def patch_copy(step, src):
        part = patches.at[pl.ds(pl.multiple_of(src * fdim, fdim), fdim)]
        return remote(
            part, part, patch_send.at[step], patch_recv.at[src], protos=lax.rem(p + step, n_protos)
        )

    def row_copy(it, step):
        return remote(
            row_out.at[it], row_in.at[it, step], row_send.at[it, step], row_recv.at[it, step],
            protos=lax.rem(p + step, n_protos),
        )

    def mass_copy(it, step):
        return remote(
            mass_out.at[it], mass_in.at[it, step], mass_send.at[it, step], mass_recv.at[it, step],
            rows=lax.rem(r + step, n_rows),
        )

    def scale_copy(step, src):
        return remote(
            scales.at[src], scales.at[src], scale_send.at[step], scale_recv.at[src],
            rows=lax.rem(r + step, n_rows),
        )

    feat_load = pltpu.make_async_copy(feat_ref, feat_in, in_sem.at[0])
    index_load = pltpu.make_async_copy(index_ref, index, in_sem.at[1])
    feat_load.start()
    index_load.start()
    each(chunks, lambda c: own_copy(c).start())

    barrier = pltpu.get_barrier_semaphore()

    def greet(semaphore, **device):
        pl.semaphore_signal(semaphore, inc=1, device_id=device, device_id_type=mesh_id)

    greet(barrier, rows=other)
    when(z > 0, lambda: greet(barrier, rows=r - 2))
    when(z < nz - 1, lambda: greet(barrier, rows=r + 2))
    for step in range(1, n_protos):
        greet(barrier, protos=lax.rem(p + step, n_protos))

    onehot[...] = jnp.zeros_like(onehot)
    index_load.wait()
    hits = lax.broadcasted_iota(jnp.int32, (onehot.shape[0], rows), 0) == index[...]
    onehot[:, :rows] = hits.astype(jnp.float32).astype(jnp.bfloat16)
    feat_load.wait()
    picked = jnp.dot(feat_in[...], onehot[...], preferred_element_type=jnp.float32)
    picked = jnp.where(odd, pltpu.roll(picked, 2 * BLOCK - rows, 1), picked)
    picks[0] = picked.astype(jnp.bfloat16)
    acc[...] = jnp.zeros_like(acc)
    each(chunks, lambda c: own_copy(c).wait())

    def order(way, k):
        if way == ACROSS:
            swapped = jnp.where(both(k >= EARLY_AT, k <= EARLY_AT + 1), 2 * EARLY_AT + 1 - k, k)
            return jnp.where(z < nz // 2, chunks - 1 - k, swapped)
        return k if way == UP else chunks - 1 - k

    def lead(way):
        behind = z if way == UP else nz - 1 - z
        count = LEAD_Z[nz - 1]
        for at in range(nz - 1):
            count = jnp.where(behind == at, LEAD_Z[at], count)
        return count

    def own_line(way, k):
        c = order(way, k)
        more = (goes_up if way == UP else goes_down)(c, True)
        when(both(k < chunks, more), lambda: block_copy(way, r, c).start())

    def own_across(k):
        c = order(ACROSS, k)
        when(both(k < chunks, owner(c) != other), lambda: block_copy(ACROSS, r, c).start())

    def hear(sem, behind, ahead_there, ahead):
        when(behind, lambda: pl.semaphore_wait(sem, 1))
        when(ahead_there, lambda: greet(sem, rows=ahead))

    def hear_up():
        hear(line_sem.at[UP], z > 0, z < nz - 1, r + 2)

    def hear_down():
        hear(line_sem.at[DOWN], z < nz - 1, z > 0, r - 2)

    met = n_protos - 1 + 1 + jnp.where(z > 0, 1, 0) + jnp.where(z < nz - 1, 1, 0)
    pl.semaphore_wait(barrier, met)
    pick_across().start()
    for way in (DOWN, UP):
        for k in range(FIRST_Z):
            own_line(way, k)
    for j in range(SPLIT):
        block_copy(ACROSS, r, other * SPLIT + j).start()
    for k in range(FIRST_Y):
        own_across(k)

    @pl.when(z < nz // 2)
    def _():
        hear_up()
        hear_down()

    @pl.when(z >= nz // 2)
    def _():
        hear_down()
        hear_up()

    pick_across().wait()
    mine = picks[0].astype(jnp.float32)
    theirs = picks[1].astype(jnp.float32)
    even = jnp.where(odd, theirs, mine)
    uneven = jnp.where(odd, mine, theirs)
    pairs[z, :, :BLOCK] = even[:, :BLOCK].astype(jnp.bfloat16)
    pairs[z, :, BLOCK:2 * BLOCK] = (even[:, BLOCK:] + uneven[:, :BLOCK]).astype(jnp.bfloat16)
    pairs[z, :, 2 * BLOCK:] = uneven[:, BLOCK:].astype(jnp.bfloat16)
    for step in range(1, nz):
        pick_copy(step, z).start()
    for apart in range(1, nz):
        for side in (1, -1):
            there = both(z + side * apart >= 0, z + side * apart < nz)
            for c in range(2 * SPLIT):
                when(there, lambda: direct_copy(lax.rem(nz + side * apart, nz), c).start())
    for way in (DOWN, UP):
        each(lead(way) - FIRST_Z, lambda k: own_line(way, k + FIRST_Z))

    each(LEAD_Y - FIRST_Y, lambda k: own_across(k + FIRST_Y))

    def spread_picks():
        for step in range(1, nz):
            pick_copy(step, lax.rem(z + step, nz)).wait_recv()
        mine = pl.ds(pl.multiple_of(p * fdim, fdim), fdim)
        for j in range(nz):
            patches[mine, 3 * BLOCK * j:3 * BLOCK * (j + 1)] = pairs[j]
        for step in range(1, n_protos):
            patch_copy(step, p).start()

    def relay():
        for apart in range(1, nz):
            for side in (1, -1):
                ahead = z + side * apart
                src = ahead * 2 + y

                @pl.when(both(ahead >= 0, ahead < nz))
                def _():
                    for j in range(SPLIT):
                        block_copy(ACROSS, src, other * SPLIT + j).wait_recv()
                        block_copy(ACROSS, src, other * SPLIT + j).start()
                    for j in range(SPLIT):
                        block_copy(ACROSS, src, r * SPLIT + j).wait_recv()

    def take_patches():
        for step in range(1, n_protos):
            patch_copy(step, lax.rem(p + step, n_protos)).wait_recv()
        pair[...] = patches[:, pl.ds(pl.multiple_of(z * (2 * rows), 2 * rows), 2 * rows)].T
        chosen[...] = pair[pl.ds(pl.multiple_of(y * rows, rows), rows), :]
        wide = chosen[...].astype(jnp.float32)
        scale = lax.rsqrt(jnp.sum(wide * wide, axis=1, keepdims=True) + EPS)
        feat_scale[...] = jnp.broadcast_to(scale * (LOG2E / TEMP), feat_scale.shape)
        for t in range(lanes // BLOCK):
            wide = patches[:, t * BLOCK:(t + 1) * BLOCK].astype(jnp.float32)
            scale = lax.rsqrt(jnp.sum(wide * wide, axis=0, keepdims=True) + EPS)
            lane_scale[:, t * BLOCK:(t + 1) * BLOCK] = scale * (LOG2E / TEMP)

    def take_own():
        for step in range(nz):
            src = lax.rem(other + 2 * step, n_rows)
            apart = jnp.abs(src // 2 - z)
            for j in range(SPLIT):
                c = r * SPLIT + j
                k = jnp.where(src // 2 > z, order(DOWN, c), c)
                at = jnp.where(early(c), EARLY_AT + apart, k + nz - 1)
                at = jnp.where(apart == 0, order(ACROSS, c), at)
                when(at > STATS_AT, lambda: block_copy(ACROSS, src, c).wait_recv())

    def turned(column):
        return jnp.broadcast_to(column, (BLOCK, BLOCK)).T[:1]

    def add_rows(value, col_mass):
        col_scale = 1.0 / (protos_all * col_mass)
        scaled = (value * col_scale).reshape(value.shape[0] // 8, 8, lanes)
        acc[...] += jnp.sum(scaled, axis=0)
        return col_scale

    def make_weights(part):
        count = width // TILE // PARTS

        def body(i):
            tile = part * count + i
            per = span // TILE
            within = pl.ds(pl.multiple_of(lax.rem(tile, per) * TILE, TILE), TILE)
            block = full[r * SPLIT + tile // per, :, within].T
            wide = block.astype(jnp.float32)
            proto_scale = lax.rsqrt(jnp.sum(wide * wide, axis=1, keepdims=True) + EPS)
            raw = jnp.dot(block, patches[...], preferred_element_type=jnp.float32)
            value = jnp.exp2(raw * lane_scale[...] * proto_scale)
            weights[pl.ds(pl.multiple_of(tile * TILE, TILE), TILE)] = value
            add_rows(value, jnp.sum(value, axis=1, keepdims=True))
            for j in range(TILE // BLOCK):
                at = pl.ds(pl.multiple_of(tile * TILE + j * BLOCK, BLOCK), BLOCK)
                scales[r, 1, :, at] = turned(proto_scale[j * BLOCK:(j + 1) * BLOCK])

        each(count, body)

    def one_pass(it):
        def body(tile):
            at = pl.ds(pl.multiple_of(tile * BLOCK, BLOCK), BLOCK)
            value = weights[at]
            col_mass = jnp.sum(value * row_scale[...], axis=1, keepdims=True)
            col_scale = add_rows(value, col_mass)
            if it == ITERS - 1:
                scales[r, 0, :, at] = turned(col_scale)

        each(width // BLOCK, body)

    def give_rows(it):
        row_out[it] = jnp.sum(acc[...], axis=0, keepdims=True)
        acc[...] = jnp.zeros_like(acc)
        for step in range(1, n_protos):
            row_copy(it, step).start()

    def give_mass(it):
        mass = row_out[it]
        for step in range(1, n_protos):
            row_copy(it, step).wait_recv()
            mass = mass + row_in[it, step]
        mass_out[it] = mass
        for step in range(1, n_rows):
            mass_copy(it, step).start()

    def take_mass(it):
        mass = mass_out[it]
        for step in range(1, n_rows):
            mass_copy(it, step).wait_recv()
            mass = mass + mass_in[it, step]
        row_scale[...] = 1.0 / (masked * mass)

    def next_pass(it):
        take_mass(it - 1)
        one_pass(it)
        if it == ITERS - 1:
            for step in range(1, n_rows):
                scale_copy(step, r).start()
        give_rows(it)

    def settle():
        take_mass(ITERS - 1)
        at = lax.broadcasted_iota(jnp.int32, (rows, lanes), 1)
        row = lax.broadcasted_iota(jnp.int32, (rows, lanes), 0) + r * rows
        found = jnp.where(at == row, jnp.broadcast_to(row_scale[...], (rows, lanes)), 0.0)
        found = jnp.sum(found, axis=1, keepdims=True) * (protos_all * masked)
        out_scale[...] = jnp.broadcast_to(found, out_scale.shape)
        for step in range(1, n_rows):
            scale_copy(step, lax.rem(r + step, n_rows)).wait_recv()

    def make_output(c):
        tile = min(512, span)
        for t in range(span // tile):
            block = full[c, :, t * tile:(t + 1) * tile]
            raw = jnp.dot(chosen[...], block, preferred_element_type=jnp.float32)
            at = pl.ds(pl.multiple_of(lax.rem(c, SPLIT) * span + t * tile, tile), tile)
            value = jnp.exp2(raw * feat_scale[:, :1] * scales[owner(c), 1, :, at])
            value = out_scale[:, :1] * value * scales[owner(c), 0, :, at]
            out_ref[c, :, t * tile:(t + 1) * tile] = value.astype(jnp.bfloat16)

    work = (
        spread_picks,
        relay,
        take_patches,
        take_own,
        lambda: make_weights(0),
        lambda: (make_weights(1), give_rows(0)),
        lambda: give_mass(0),
        lambda: next_pass(1),
        lambda: give_mass(1),
        lambda: next_pass(2),
        lambda: give_mass(2),
        settle,
    )
    first = (STAGES[-1] + 1) // 4

    def hooks(i, place):
        for at, stage in zip(STAGES, work):
            if at % 4 == place:
                when(i == at // 4, stage)

    pace = 4

    def beside(i):
        c = order(ACROSS, i)
        src = other
        when(jnp.logical_or(owner(c) != r, i <= STATS_AT), lambda: block_copy(ACROSS, src, c).wait_recv())
        when(both(early(c), goes_up(c, False)), lambda: block_copy(UP, src, c).start())
        when(both(early(c), goes_down(c, False)), lambda: block_copy(DOWN, src, c).start())

    def ways(d):
        return (
            (DOWN, z + d, goes_down, z + d < nz),
            (UP, z - d, goes_up, z - d >= 0),
        )

    def line(i, k, d):
        for way, ahead, more, there in ways(d):
            src = ahead * 2 + y
            c = order(way, k)

            @pl.when(there)
            def _():
                when(plane(c) != z, lambda: block_copy(ACROSS, src, c).wait_recv())
                when(more(c, True), lambda: block_copy(way, src, c).start())
                when(
                    both(no(early(c)), owner(c) != other), lambda: block_copy(ACROSS, src, c).start()
                )

    def take_far(i, src, c):
        when(
            jnp.logical_or(owner(c) != r, i <= STATS_AT),
            lambda: block_copy(ACROSS, src, c).wait_recv(),
        )

    def early_line(i, d):
        for way, ahead, more, there in ways(d):
            src = ahead * 2 + 1 - y

            @pl.when(there)
            def _():
                for c in EARLY:
                    take_far(i, src, c)
                    when(more(c, False), lambda: block_copy(way, src, c).start())

    def far_line(i, k, d):
        for way, ahead, more, there in ways(d):
            c = order(way, k)
            when(both(there, no(early(c))), lambda: take_far(i, ahead * 2 + 1 - y, c))

    def drain(k):
        across = order(ACROSS, k)
        block_copy(ACROSS, r, across).wait_send()
        for way in (DOWN, UP):
            c = order(way, k)
            for d in range(nz):
                ahead = z + d if way == DOWN else z - d
                more = goes_down(c, True) if way == DOWN else goes_up(c, True)
                there = ahead < nz if way == DOWN else ahead >= 0

                @pl.when(there)
                def _():
                    src = ahead * 2 + y
                    when(more, lambda: block_copy(way, src, c).wait_send())
                    if d > 0:
                        when(
                            jnp.logical_or(no(early(c)), owner(c) == other),
                            lambda: block_copy(ACROSS, src, c).wait_send(),
                        )

    def drain_early():
        for c in EARLY:
            for way in (DOWN, UP):
                for d in range(nz):
                    ahead = z + d if way == DOWN else z - d
                    more = goes_down(c, False) if way == DOWN else goes_up(c, False)
                    there = ahead < nz if way == DOWN else ahead >= 0
                    src = ahead * 2 + 1 - y
                    when(both(there, more), lambda: block_copy(way, src, c).wait_send())

    middle = both(z > 0, z < nz - 1)

    def ready(i):
        last = i - nz + 1
        return jnp.where(middle, 2 * last - chunks, last)

    def done_by(i):
        return jnp.clip(jnp.minimum((i - first + 1) * pace, ready(i)), 0, chunks)

    def nth(k):
        half = chunks // 2
        inner = jnp.where(k % 2 == 0, half - 1 - k // 2, half + k // 2)
        return jnp.where(middle, inner, jnp.where(z == 0, chunks - 1 - k, k))

    def output(k, carry):
        make_output(nth(k))
        return carry

    def step_of(i, carry):
        for way in (DOWN, UP):
            own_line(way, i + lead(way))
        own_across(i + LEAD_Y)
        when(i < chunks, lambda: beside(i))
        hooks(i, 0)
        for d in range(1, nz):
            k = i - (d - 1)
            when(both(k >= 0, k < chunks), lambda: line(i, k, d))
            if d < nz - 1:
                hooks(i, d)
            if d == nz - 2:
                lax.fori_loop(done_by(i - 1), done_by(i), output, 0)
        for d in range(1, nz):
            when(i == EARLY_AT + d, lambda: early_line(i, d))
        last = i - (nz - 1)

        @pl.when(last >= 0)
        def _():
            for d in range(1, nz):
                far_line(i, last, d)

        hooks(i, 3)

        when(last >= LAG, lambda: drain(last - LAG))
        return carry

    steps = chunks + nz - 1
    lax.fori_loop(0, steps, step_of, 0)
    lax.fori_loop(done_by(steps - 1), chunks, output, 0)

    for step in range(1, nz):
        pick_copy(step, z).wait_send()
    for step in range(1, n_rows):
        scale_copy(step, r).wait_send()
    for step in range(1, nz):
        for c in range(2 * SPLIT):
            direct_copy(step, c).wait_send()
    for step in range(1, n_protos):
        patch_copy(step, p).wait_send()
    for it in range(ITERS):
        for step in range(1, n_rows):
            mass_copy(it, step).wait_send()
        for step in range(1, n_protos):
            row_copy(it, step).wait_send()

    def rest(i, carry):
        drain(i)
        return carry

    lax.fori_loop(chunks - LAG, chunks, rest, 0)
    drain_early()


def finish(blocks_ref, out_ref, out_sem):
    count, rows, span = blocks_ref.shape
    copies = [
        pltpu.make_async_copy(
            blocks_ref.at[c], out_ref.at[:, c * span:(c + 1) * span], out_sem.at[c]
        )
        for c in range(count)
    ]
    for copy in copies:
        copy.start()
    for copy in copies:
        copy.wait()


def with_kernel(n_rows, n_protos, features, prototypes, masked_index):
    rows = masked_index.shape[0]
    dim, total = prototypes.shape[1], prototypes.shape[0]
    fdim, patches = features.shape[1], features.shape[0]
    width = total // n_rows
    chunks = n_rows * SPLIT
    span = total // chunks
    lanes = rows * n_rows
    depth = fdim * n_protos
    masked = float(lanes)
    protos_all = float(total * n_protos)
    f32, bf16, dma = jnp.float32, jnp.bfloat16, pltpu.SemaphoreType.DMA
    vmem = pl.BlockSpec(memory_space=pltpu.VMEM)
    anywhere = pl.BlockSpec(memory_space=pl.ANY)
    blocks = pl.pallas_call(
        functools.partial(kernel, n_rows, n_protos, masked, protos_all),
        out_shape=jax.ShapeDtypeStruct((chunks, rows, span), bf16),
        in_specs=[pl.BlockSpec(memory_space=pltpu.HBM)] * 3,
        out_specs=vmem,
        scratch_shapes=[
            pltpu.VMEM((fdim, patches), bf16),
            pltpu.VMEM((1, rows), jnp.int32),
            pltpu.VMEM((patches, 2 * BLOCK), bf16),
            pltpu.VMEM((2, fdim, 2 * BLOCK), bf16),
            pltpu.VMEM((n_rows // 2, fdim, 3 * BLOCK), bf16),
            pltpu.VMEM((depth, lanes), bf16),
            pltpu.VMEM((2 * rows, depth), bf16),
            pltpu.VMEM((rows, depth), bf16),
            pltpu.VMEM((1, lanes), f32),
            pltpu.VMEM((rows, BLOCK), f32),
            pltpu.VMEM((chunks, dim * n_rows, span), bf16),
            pltpu.VMEM((width, lanes), f32),
            pltpu.VMEM((8, lanes), f32),
            pltpu.VMEM((ITERS, 1, lanes), f32),
            pltpu.VMEM((ITERS, n_protos, 1, lanes), f32),
            pltpu.VMEM((ITERS, 1, lanes), f32),
            pltpu.VMEM((ITERS, n_rows, 1, lanes), f32),
            pltpu.VMEM((1, lanes), f32),
            pltpu.VMEM((rows, BLOCK), f32),
            pltpu.VMEM((n_rows, 2, 1, width), f32),
            pltpu.SemaphoreType.REGULAR((2,)),
            dma((2,)),
            dma((chunks,)),
            dma((n_rows,)),
            dma((n_rows,)),
            dma((n_protos,)),
            dma((n_protos,)),
            dma((3, n_rows, chunks)),
            dma((n_rows, chunks)),
            dma((n_rows // 2, 2 * SPLIT)),
            dma((ITERS, n_protos)),
            dma((ITERS, n_protos)),
            dma((ITERS, n_rows)),
            dma((ITERS, n_rows)),
            dma((n_rows,)),
            dma((n_rows,)),
        ],
        compiler_params=pltpu.CompilerParams(
            collective_id=0, has_side_effects=True, vmem_limit_bytes=46 * 1024 * 1024
        ),
    )(*(pltpu.with_memory_space_constraint(x, pltpu.HBM) for x in (features.T, prototypes.T, masked_index[None, :])))
    return pl.pallas_call(
        finish,
        out_shape=jax.ShapeDtypeStruct((rows, total), bf16),
        in_specs=[vmem],
        out_specs=anywhere,
        scratch_shapes=[dma((chunks,))],
        compiler_params=pltpu.CompilerParams(vmem_limit_bytes=4 * 1024 * 1024),
    )(blocks)


def with_collectives(features, prototypes, masked_index):
    total_protos = float(prototypes.shape[0] * lax.axis_size("protos"))
    chosen = jnp.take(features, masked_index, axis=0)
    patches = lax.all_gather(chosen, "protos", axis=1, tiled=True)
    feat_scale = lax.rsqrt(jnp.sum(jnp.square(patches.astype(jnp.float32)), axis=1) + EPS)
    full = lax.all_gather(prototypes, "rows", axis=1, tiled=True)
    proto_sq = jnp.sum(jnp.square(full.astype(jnp.float32)), axis=1)
    raw = lax.dot_general(
        patches, full, (((1,), (1,)), ((), ())), preferred_element_type=jnp.float32
    )
    proto_scale = lax.rsqrt(proto_sq + EPS)
    weights = jnp.exp(raw * feat_scale[:, None] * proto_scale[None, :] / TEMP)
    total_rows = masked_index.shape[0] * lax.axis_size("rows")
    row_scale = jnp.ones((patches.shape[0],), jnp.float32)
    for step in range(ITERS):
        col_part = jnp.dot(row_scale, weights, precision=lax.Precision.HIGHEST)
        col_scale = 1.0 / (total_protos * lax.psum(col_part, "rows"))
        row_part = jnp.dot(weights, col_scale, precision=lax.Precision.HIGHEST)
        row_scale = 1.0 / (total_rows * lax.psum(row_part, "protos"))
    factor = total_protos * float(total_rows)
    return (factor * row_scale[:, None] * weights * col_scale[None, :]).astype(jnp.bfloat16)


def solution(mesh):
    n_rows, n_protos = mesh.shape["rows"], mesh.shape["protos"]
    in_specs = (P("rows", "protos"), P("protos", "rows"), P("rows"))
    out_specs = P("rows", "protos")

    def on_device(features, prototypes, masked_index):
        fits = (
            n_rows % 2 == 0
            and n_rows == 8
            and n_protos > 1
            and prototypes.shape[1] % 16 == 0
            and features.shape[1] % 16 == 0
            and features.shape[1] * n_protos == prototypes.shape[1] * n_rows
            and 2 * masked_index.shape[0] == 3 * BLOCK
            and prototypes.shape[0] % (n_rows * SPLIT * 512) == 0
        )
        if fits:
            return with_kernel(n_rows, n_protos, features, prototypes, masked_index)
        return with_collectives(features, prototypes, masked_index)

    return jax.shard_map(
        on_device, mesh=mesh, in_specs=in_specs, out_specs=out_specs, check_vma=False
    )
```

```python
import functools

import jax
import jax.numpy as jnp
from jax import lax
from jax.experimental import pallas as pl
from jax.experimental.pallas import tpu as pltpu
from jax.sharding import PartitionSpec as P

ITERS = 3


TEMP = 0.07
EPS = 1e-06
LOG2E = 1.4426950408889634
UP, DOWN, ACROSS = 0, 1, 2
LEAD_Z = (3, 2, 4, 0)
LEAD_Y = 8
FIRST_Z = 1
FIRST_Y = 2
SPLIT = 1
EARLY = (4,)
EARLY_AT = 3
LAG = 2
STATS_AT = 1
STAGES = (3, 3, 6, 7, 8, 9, 11, 15, 17, 21, 23, 28)
BLOCK = 128
TILE = 512
PARTS = 2


def kernel(
    n_rows, n_protos, masked, protos_all,
    feat_ref, proto_ref, index_ref, out_ref,
    feat_in, index, onehot, picks, pairs, patches, pair, chosen, lane_scale, feat_scale, full, weights,
    acc, row_out, row_in, mass_out, mass_in, row_scale, out_scale, scales,
    line_sem, in_sem, own_sem, pick_send, pick_recv, patch_send, patch_recv, send, recv, direct_send,
    row_send, row_recv, mass_send, mass_recv, scale_send, scale_recv,
):
    r, p = lax.axis_index("rows"), lax.axis_index("protos")
    z, y = r // 2, lax.rem(r, 2)
    nz = n_rows // 2
    other = z * 2 + 1 - y
    dim, total = proto_ref.shape
    width = total // n_rows
    chunks = n_rows * SPLIT
    span = total // chunks
    rows = index_ref.shape[1]
    fdim = feat_ref.shape[0]
    lanes = rows * n_rows
    odd = y == 1
    both = jnp.logical_and
    no = jnp.logical_not
    mesh_id = pl.DeviceIdType.MESH

    def where(src, c):
        return full.at[c, pl.ds(pl.multiple_of(src * dim, dim), dim)]

    def own_copy(c):
        return pltpu.make_async_copy(
            proto_ref.at[:, pl.ds(pl.multiple_of(c * span, span), span)], where(r, c), own_sem.at[c]
        )

    def early(c):
        hit = c == EARLY[0]
        for e in EARLY[1:]:
            hit = jnp.logical_or(hit, c == e)
        return hit

    def owner(c):
        return c // SPLIT

    def plane(c):
        return c // (2 * SPLIT)

    def remote(src, dst, send_sem, recv_sem, **device):
        return pltpu.make_async_remote_copy(
            src_ref=src, dst_ref=dst, send_sem=send_sem, recv_sem=recv_sem,
            device_id=device, device_id_type=mesh_id,
        )

    def block_copy(way, src, c):
        target = {UP: r + 2, DOWN: r - 2, ACROSS: other}[way]
        return remote(where(src, c), where(src, c), send.at[way, src, c], recv.at[src, c], rows=target)

    def when(condition, action):
        @pl.when(condition)
        def _():
            action()

    def each(count, body):
        def step(i, carry):
            body(i)
            return carry

        lax.fori_loop(0, count, step, 0)

    def goes_up(c, on_line):
        return both(z < nz - 1, plane(c) != z + 1 if on_line else owner(c) != r + 2)

    def goes_down(c, on_line):
        return both(z > 0, plane(c) != z - 1 if on_line else owner(c) != r - 2)

    def direct_copy(step, c):
        target = lax.rem(r + 2 * step, n_rows)
        chunk = target // 2 * (2 * SPLIT) + c
        return remote(
            where(r, chunk), where(r, chunk), direct_send.at[step, c], recv.at[r, chunk], rows=target
        )

    def pick_across():
        return remote(picks.at[0], picks.at[1], pick_send.at[0], pick_recv.at[nz], rows=other)

    def pick_copy(step, src):
        return remote(
            pairs.at[src], pairs.at[src], pick_send.at[step], pick_recv.at[src],
            rows=lax.rem(r + 2 * step, n_rows),
        )

    def patch_copy(step, src):
        part = patches.at[pl.ds(pl.multiple_of(src * fdim, fdim), fdim)]
        return remote(
            part, part, patch_send.at[step], patch_recv.at[src], protos=lax.rem(p + step, n_protos)
        )

    def row_copy(it, step):
        return remote(
            row_out.at[it], row_in.at[it, step], row_send.at[it, step], row_recv.at[it, step],
            protos=lax.rem(p + step, n_protos),
        )

    def mass_copy(it, step):
        return remote(
            mass_out.at[it], mass_in.at[it, step], mass_send.at[it, step], mass_recv.at[it, step],
            rows=lax.rem(r + step, n_rows),
        )

    def scale_copy(step, src):
        return remote(
            scales.at[src], scales.at[src], scale_send.at[step], scale_recv.at[src],
            rows=lax.rem(r + step, n_rows),
        )

    feat_load = pltpu.make_async_copy(feat_ref, feat_in, in_sem.at[0])
    index_load = pltpu.make_async_copy(index_ref, index, in_sem.at[1])
    feat_load.start()
    index_load.start()
    each(chunks, lambda c: own_copy(c).start())

    barrier = pltpu.get_barrier_semaphore()

    def greet(semaphore, **device):
        pl.semaphore_signal(semaphore, inc=1, device_id=device, device_id_type=mesh_id)

    greet(barrier, rows=other)
    when(z > 0, lambda: greet(barrier, rows=r - 2))
    when(z < nz - 1, lambda: greet(barrier, rows=r + 2))
    for step in range(1, n_protos):
        greet(barrier, protos=lax.rem(p + step, n_protos))

    onehot[...] = jnp.zeros_like(onehot)
    index_load.wait()
    hits = lax.broadcasted_iota(jnp.int32, (onehot.shape[0], rows), 0) == index[...]
    onehot[:, :rows] = hits.astype(jnp.float32).astype(jnp.bfloat16)
    feat_load.wait()
    picked = jnp.dot(feat_in[...], onehot[...], preferred_element_type=jnp.float32)
    picked = jnp.where(odd, pltpu.roll(picked, 2 * BLOCK - rows, 1), picked)
    picks[0] = picked.astype(jnp.bfloat16)
    acc[...] = jnp.zeros_like(acc)
    each(chunks, lambda c: own_copy(c).wait())

    def order(way, k):
        if way == ACROSS:
            swapped = jnp.where(both(k >= EARLY_AT, k <= EARLY_AT + 1), 2 * EARLY_AT + 1 - k, k)
            return jnp.where(z < nz // 2, chunks - 1 - k, swapped)
        return k if way == UP else chunks - 1 - k

    def lead(way):
        behind = z if way == UP else nz - 1 - z
        count = LEAD_Z[nz - 1]
        for at in range(nz - 1):
            count = jnp.where(behind == at, LEAD_Z[at], count)
        return count

    def own_line(way, k):
        c = order(way, k)
        more = (goes_up if way == UP else goes_down)(c, True)
        when(both(k < chunks, more), lambda: block_copy(way, r, c).start())

    def own_across(k):
        c = order(ACROSS, k)
        when(both(k < chunks, owner(c) != other), lambda: block_copy(ACROSS, r, c).start())

    def hear(sem, behind, ahead_there, ahead):
        when(behind, lambda: pl.semaphore_wait(sem, 1))
        when(ahead_there, lambda: greet(sem, rows=ahead))

    def hear_up():
        hear(line_sem.at[UP], z > 0, z < nz - 1, r + 2)

    def hear_down():
        hear(line_sem.at[DOWN], z < nz - 1, z > 0, r - 2)

    met = n_protos - 1 + 1 + jnp.where(z > 0, 1, 0) + jnp.where(z < nz - 1, 1, 0)
    pl.semaphore_wait(barrier, met)
    pick_across().start()
    for way in (DOWN, UP):
        for k in range(FIRST_Z):
            own_line(way, k)
    for j in range(SPLIT):
        block_copy(ACROSS, r, other * SPLIT + j).start()
    for k in range(FIRST_Y):
        own_across(k)

    @pl.when(z < nz // 2)
    def _():
        hear_up()
        hear_down()

    @pl.when(z >= nz // 2)
    def _():
        hear_down()
        hear_up()

    pick_across().wait()
    mine = picks[0].astype(jnp.float32)
    theirs = picks[1].astype(jnp.float32)
    even = jnp.where(odd, theirs, mine)
    uneven = jnp.where(odd, mine, theirs)
    pairs[z, :, :BLOCK] = even[:, :BLOCK].astype(jnp.bfloat16)
    pairs[z, :, BLOCK:2 * BLOCK] = (even[:, BLOCK:] + uneven[:, :BLOCK]).astype(jnp.bfloat16)
    pairs[z, :, 2 * BLOCK:] = uneven[:, BLOCK:].astype(jnp.bfloat16)
    for step in range(1, nz):
        pick_copy(step, z).start()
    for apart in range(1, nz):
        for side in (1, -1):
            there = both(z + side * apart >= 0, z + side * apart < nz)
            for c in range(2 * SPLIT):
                when(there, lambda: direct_copy(lax.rem(nz + side * apart, nz), c).start())
    for way in (DOWN, UP):
        each(lead(way) - FIRST_Z, lambda k: own_line(way, k + FIRST_Z))

    each(LEAD_Y - FIRST_Y, lambda k: own_across(k + FIRST_Y))

    def spread_picks():
        for step in range(1, nz):
            pick_copy(step, lax.rem(z + step, nz)).wait_recv()
        mine = pl.ds(pl.multiple_of(p * fdim, fdim), fdim)
        for j in range(nz):
            patches[mine, 3 * BLOCK * j:3 * BLOCK * (j + 1)] = pairs[j]
        for step in range(1, n_protos):
            patch_copy(step, p).start()

    def relay():
        for apart in range(1, nz):
            for side in (1, -1):
                ahead = z + side * apart
                src = ahead * 2 + y

                @pl.when(both(ahead >= 0, ahead < nz))
                def _():
                    for j in range(SPLIT):
                        block_copy(ACROSS, src, other * SPLIT + j).wait_recv()
                        block_copy(ACROSS, src, other * SPLIT + j).start()
                    for j in range(SPLIT):
                        block_copy(ACROSS, src, r * SPLIT + j).wait_recv()

    def take_patches():
        for step in range(1, n_protos):
            patch_copy(step, lax.rem(p + step, n_protos)).wait_recv()
        pair[...] = patches[:, pl.ds(pl.multiple_of(z * (2 * rows), 2 * rows), 2 * rows)].T
        chosen[...] = pair[pl.ds(pl.multiple_of(y * rows, rows), rows), :]
        wide = chosen[...].astype(jnp.float32)
        scale = lax.rsqrt(jnp.sum(wide * wide, axis=1, keepdims=True) + EPS)
        feat_scale[...] = jnp.broadcast_to(scale * (LOG2E / TEMP), feat_scale.shape)
        for t in range(lanes // BLOCK):
            wide = patches[:, t * BLOCK:(t + 1) * BLOCK].astype(jnp.float32)
            scale = lax.rsqrt(jnp.sum(wide * wide, axis=0, keepdims=True) + EPS)
            lane_scale[:, t * BLOCK:(t + 1) * BLOCK] = scale * (LOG2E / TEMP)

    def take_own():
        for step in range(nz):
            src = lax.rem(other + 2 * step, n_rows)
            apart = jnp.abs(src // 2 - z)
            for j in range(SPLIT):
                c = r * SPLIT + j
                k = jnp.where(src // 2 > z, order(DOWN, c), c)
                at = jnp.where(early(c), EARLY_AT + apart, k + nz - 1)
                at = jnp.where(apart == 0, order(ACROSS, c), at)
                when(at > STATS_AT, lambda: block_copy(ACROSS, src, c).wait_recv())

    def turned(column):
        return jnp.broadcast_to(column, (BLOCK, BLOCK)).T[:1]

    def add_rows(value, col_mass):
        col_scale = 1.0 / (protos_all * col_mass)
        scaled = (value * col_scale).reshape(value.shape[0] // 8, 8, lanes)
        acc[...] += jnp.sum(scaled, axis=0)
        return col_scale

    def make_weights(part):
        count = width // TILE // PARTS

        def body(i):
            tile = part * count + i
            per = span // TILE
            within = pl.ds(pl.multiple_of(lax.rem(tile, per) * TILE, TILE), TILE)
            block = full[r * SPLIT + tile // per, :, within].T
            wide = block.astype(jnp.float32)
            proto_scale = lax.rsqrt(jnp.sum(wide * wide, axis=1, keepdims=True) + EPS)
            raw = jnp.dot(block, patches[...], preferred_element_type=jnp.float32)
            value = jnp.exp2(raw * lane_scale[...] * proto_scale)
            weights[pl.ds(pl.multiple_of(tile * TILE, TILE), TILE)] = value
            add_rows(value, jnp.sum(value, axis=1, keepdims=True))
            for j in range(TILE // BLOCK):
                at = pl.ds(pl.multiple_of(tile * TILE + j * BLOCK, BLOCK), BLOCK)
                scales[r, 1, :, at] = turned(proto_scale[j * BLOCK:(j + 1) * BLOCK])

        each(count, body)

    def one_pass(it):
        def body(tile):
            at = pl.ds(pl.multiple_of(tile * BLOCK, BLOCK), BLOCK)
            value = weights[at]
            col_mass = jnp.sum(value * row_scale[...], axis=1, keepdims=True)
            col_scale = add_rows(value, col_mass)
            if it == ITERS - 1:
                scales[r, 0, :, at] = turned(col_scale)

        each(width // BLOCK, body)

    def give_rows(it):
        row_out[it] = jnp.sum(acc[...], axis=0, keepdims=True)
        acc[...] = jnp.zeros_like(acc)
        for step in range(1, n_protos):
            row_copy(it, step).start()

    def give_mass(it):
        mass = row_out[it]
        for step in range(1, n_protos):
            row_copy(it, step).wait_recv()
            mass = mass + row_in[it, step]
        mass_out[it] = mass
        for step in range(1, n_rows):
            mass_copy(it, step).start()

    def take_mass(it):
        mass = mass_out[it]
        for step in range(1, n_rows):
            mass_copy(it, step).wait_recv()
            mass = mass + mass_in[it, step]
        row_scale[...] = 1.0 / (masked * mass)

    def next_pass(it):
        take_mass(it - 1)
        one_pass(it)
        if it == ITERS - 1:
            for step in range(1, n_rows):
                scale_copy(step, r).start()
        give_rows(it)

    def settle():
        take_mass(ITERS - 1)
        at = lax.broadcasted_iota(jnp.int32, (rows, lanes), 1)
        row = lax.broadcasted_iota(jnp.int32, (rows, lanes), 0) + r * rows
        found = jnp.where(at == row, jnp.broadcast_to(row_scale[...], (rows, lanes)), 0.0)
        found = jnp.sum(found, axis=1, keepdims=True) * (protos_all * masked)
        out_scale[...] = jnp.broadcast_to(found, out_scale.shape)
        for step in range(1, n_rows):
            scale_copy(step, lax.rem(r + step, n_rows)).wait_recv()

    def make_output(c):
        tile = min(512, span)
        for t in range(span // tile):
            block = full[c, :, t * tile:(t + 1) * tile]
            raw = jnp.dot(chosen[...], block, preferred_element_type=jnp.float32)
            at = pl.ds(pl.multiple_of(lax.rem(c, SPLIT) * span + t * tile, tile), tile)
            value = jnp.exp2(raw * feat_scale[:, :1] * scales[owner(c), 1, :, at])
            value = out_scale[:, :1] * value * scales[owner(c), 0, :, at]
            out_ref[c, :, t * tile:(t + 1) * tile] = value.astype(jnp.bfloat16)

    work = (
        spread_picks,
        relay,
        take_patches,
        take_own,
        lambda: make_weights(0),
        lambda: (make_weights(1), give_rows(0)),
        lambda: give_mass(0),
        lambda: next_pass(1),
        lambda: give_mass(1),
        lambda: next_pass(2),
        lambda: give_mass(2),
        settle,
    )
    first = (STAGES[-1] + 1) // 4

    def hooks(i, place):
        for at, stage in zip(STAGES, work):
            if at % 4 == place:
                when(i == at // 4, stage)

    pace = 4

    def beside(i):
        c = order(ACROSS, i)
        src = other
        when(jnp.logical_or(owner(c) != r, i <= STATS_AT), lambda: block_copy(ACROSS, src, c).wait_recv())
        when(both(early(c), goes_up(c, False)), lambda: block_copy(UP, src, c).start())
        when(both(early(c), goes_down(c, False)), lambda: block_copy(DOWN, src, c).start())

    def ways(d):
        return (
            (DOWN, z + d, goes_down, z + d < nz),
            (UP, z - d, goes_up, z - d >= 0),
        )

    def line(i, k, d):
        for way, ahead, more, there in ways(d):
            src = ahead * 2 + y
            c = order(way, k)

            @pl.when(there)
            def _():
                when(plane(c) != z, lambda: block_copy(ACROSS, src, c).wait_recv())
                when(more(c, True), lambda: block_copy(way, src, c).start())
                when(
                    both(no(early(c)), owner(c) != other), lambda: block_copy(ACROSS, src, c).start()
                )

    def take_far(i, src, c):
        when(
            jnp.logical_or(owner(c) != r, i <= STATS_AT),
            lambda: block_copy(ACROSS, src, c).wait_recv(),
        )

    def early_line(i, d):
        for way, ahead, more, there in ways(d):
            src = ahead * 2 + 1 - y

            @pl.when(there)
            def _():
                for c in EARLY:
                    take_far(i, src, c)
                    when(more(c, False), lambda: block_copy(way, src, c).start())

    def far_line(i, k, d):
        for way, ahead, more, there in ways(d):
            c = order(way, k)
            when(both(there, no(early(c))), lambda: take_far(i, ahead * 2 + 1 - y, c))

    def drain(k):
        across = order(ACROSS, k)
        block_copy(ACROSS, r, across).wait_send()
        for way in (DOWN, UP):
            c = order(way, k)
            for d in range(nz):
                ahead = z + d if way == DOWN else z - d
                more = goes_down(c, True) if way == DOWN else goes_up(c, True)
                there = ahead < nz if way == DOWN else ahead >= 0

                @pl.when(there)
                def _():
                    src = ahead * 2 + y
                    when(more, lambda: block_copy(way, src, c).wait_send())
                    if d > 0:
                        when(
                            jnp.logical_or(no(early(c)), owner(c) == other),
                            lambda: block_copy(ACROSS, src, c).wait_send(),
                        )

    def drain_early():
        for c in EARLY:
            for way in (DOWN, UP):
                for d in range(nz):
                    ahead = z + d if way == DOWN else z - d
                    more = goes_down(c, False) if way == DOWN else goes_up(c, False)
                    there = ahead < nz if way == DOWN else ahead >= 0
                    src = ahead * 2 + 1 - y
                    when(both(there, more), lambda: block_copy(way, src, c).wait_send())

    middle = both(z > 0, z < nz - 1)

    def ready(i):
        last = i - nz + 1
        return jnp.where(middle, 2 * last - chunks, last)

    def done_by(i):
        return jnp.clip(jnp.minimum((i - first + 1) * pace, ready(i)), 0, chunks)

    def nth(k):
        half = chunks // 2
        inner = jnp.where(k % 2 == 0, half - 1 - k // 2, half + k // 2)
        return jnp.where(middle, inner, jnp.where(z == 0, chunks - 1 - k, k))

    def output(k, carry):
        make_output(nth(k))
        return carry

    def step_of(i, carry):
        for way in (DOWN, UP):
            own_line(way, i + lead(way))
        own_across(i + LEAD_Y)
        when(i < chunks, lambda: beside(i))
        hooks(i, 0)
        for d in range(1, nz):
            k = i - (d - 1)
            when(both(k >= 0, k < chunks), lambda: line(i, k, d))
            if d < nz - 1:
                hooks(i, d)
            if d == nz - 2:
                lax.fori_loop(done_by(i - 1), done_by(i), output, 0)
        for d in range(1, nz):
            when(i == EARLY_AT + d, lambda: early_line(i, d))
        last = i - (nz - 1)

        @pl.when(last >= 0)
        def _():
            for d in range(1, nz):
                far_line(i, last, d)

        hooks(i, 3)

        when(last >= LAG, lambda: drain(last - LAG))
        return carry

    steps = chunks + nz - 1
    lax.fori_loop(0, steps, step_of, 0)
    lax.fori_loop(done_by(steps - 1), chunks, output, 0)

    for step in range(1, nz):
        pick_copy(step, z).wait_send()
    for step in range(1, n_rows):
        scale_copy(step, r).wait_send()
    for step in range(1, nz):
        for c in range(2 * SPLIT):
            direct_copy(step, c).wait_send()
    for step in range(1, n_protos):
        patch_copy(step, p).wait_send()
    for it in range(ITERS):
        for step in range(1, n_rows):
            mass_copy(it, step).wait_send()
        for step in range(1, n_protos):
            row_copy(it, step).wait_send()

    def rest(i, carry):
        drain(i)
        return carry

    lax.fori_loop(chunks - LAG, chunks, rest, 0)
    drain_early()


def finish(blocks_ref, out_ref, out_sem):
    count, rows, span = blocks_ref.shape
    copies = [
        pltpu.make_async_copy(
            blocks_ref.at[c], out_ref.at[:, c * span:(c + 1) * span], out_sem.at[c]
        )
        for c in range(count)
    ]
    for copy in copies:
        copy.start()
    for copy in copies:
        copy.wait()


def with_kernel(n_rows, n_protos, features, prototypes, masked_index):
    rows = masked_index.shape[0]
    dim, total = prototypes.shape[1], prototypes.shape[0]
    fdim, patches = features.shape[1], features.shape[0]
    width = total // n_rows
    chunks = n_rows * SPLIT
    span = total // chunks
    lanes = rows * n_rows
    depth = fdim * n_protos
    masked = float(lanes)
    protos_all = float(total * n_protos)
    f32, bf16, dma = jnp.float32, jnp.bfloat16, pltpu.SemaphoreType.DMA
    vmem = pl.BlockSpec(memory_space=pltpu.VMEM)
    anywhere = pl.BlockSpec(memory_space=pl.ANY)
    blocks = pl.pallas_call(
        functools.partial(kernel, n_rows, n_protos, masked, protos_all),
        out_shape=jax.ShapeDtypeStruct((chunks, rows, span), bf16),
        in_specs=[pl.BlockSpec(memory_space=pltpu.HBM)] * 3,
        out_specs=vmem,
        scratch_shapes=[
            pltpu.VMEM((fdim, patches), bf16),
            pltpu.VMEM((1, rows), jnp.int32),
            pltpu.VMEM((patches, 2 * BLOCK), bf16),
            pltpu.VMEM((2, fdim, 2 * BLOCK), bf16),
            pltpu.VMEM((n_rows // 2, fdim, 3 * BLOCK), bf16),
            pltpu.VMEM((depth, lanes), bf16),
            pltpu.VMEM((2 * rows, depth), bf16),
            pltpu.VMEM((rows, depth), bf16),
            pltpu.VMEM((1, lanes), f32),
            pltpu.VMEM((rows, BLOCK), f32),
            pltpu.VMEM((chunks, dim * n_rows, span), bf16),
            pltpu.VMEM((width, lanes), f32),
            pltpu.VMEM((8, lanes), f32),
            pltpu.VMEM((ITERS, 1, lanes), f32),
            pltpu.VMEM((ITERS, n_protos, 1, lanes), f32),
            pltpu.VMEM((ITERS, 1, lanes), f32),
            pltpu.VMEM((ITERS, n_rows, 1, lanes), f32),
            pltpu.VMEM((1, lanes), f32),
            pltpu.VMEM((rows, BLOCK), f32),
            pltpu.VMEM((n_rows, 2, 1, width), f32),
            pltpu.SemaphoreType.REGULAR((2,)),
            dma((2,)),
            dma((chunks,)),
            dma((n_rows,)),
            dma((n_rows,)),
            dma((n_protos,)),
            dma((n_protos,)),
            dma((3, n_rows, chunks)),
            dma((n_rows, chunks)),
            dma((n_rows // 2, 2 * SPLIT)),
            dma((ITERS, n_protos)),
            dma((ITERS, n_protos)),
            dma((ITERS, n_rows)),
            dma((ITERS, n_rows)),
            dma((n_rows,)),
            dma((n_rows,)),
        ],
        compiler_params=pltpu.CompilerParams(
            collective_id=0, has_side_effects=True, vmem_limit_bytes=46 * 1024 * 1024
        ),
    )(*(pltpu.with_memory_space_constraint(x, pltpu.HBM) for x in (features.T, prototypes.T, masked_index[None, :])))
    return pl.pallas_call(
        finish,
        out_shape=jax.ShapeDtypeStruct((rows, total), bf16),
        in_specs=[vmem],
        out_specs=anywhere,
        scratch_shapes=[dma((chunks,))],
        compiler_params=pltpu.CompilerParams(vmem_limit_bytes=4 * 1024 * 1024),
    )(blocks)


def with_collectives(features, prototypes, masked_index):
    total_protos = float(prototypes.shape[0] * lax.axis_size("protos"))
    chosen = jnp.take(features, masked_index, axis=0)
    patches = lax.all_gather(chosen, "protos", axis=1, tiled=True)
    feat_scale = lax.rsqrt(jnp.sum(jnp.square(patches.astype(jnp.float32)), axis=1) + EPS)
    full = lax.all_gather(prototypes, "rows", axis=1, tiled=True)
    proto_sq = jnp.sum(jnp.square(full.astype(jnp.float32)), axis=1)
    raw = lax.dot_general(
        patches, full, (((1,), (1,)), ((), ())), preferred_element_type=jnp.float32
    )
    proto_scale = lax.rsqrt(proto_sq + EPS)
    weights = jnp.exp(raw * feat_scale[:, None] * proto_scale[None, :] / TEMP)
    total_rows = masked_index.shape[0] * lax.axis_size("rows")
    row_scale = jnp.ones((patches.shape[0],), jnp.float32)
    for step in range(ITERS):
        col_part = jnp.dot(row_scale, weights, precision=lax.Precision.HIGHEST)
        col_scale = 1.0 / (total_protos * lax.psum(col_part, "rows"))
        row_part = jnp.dot(weights, col_scale, precision=lax.Precision.HIGHEST)
        row_scale = 1.0 / (total_rows * lax.psum(row_part, "protos"))
    factor = total_protos * float(total_rows)
    return (factor * row_scale[:, None] * weights * col_scale[None, :]).astype(jnp.bfloat16)


def solution(mesh):
    n_rows, n_protos = mesh.shape["rows"], mesh.shape["protos"]
    in_specs = (P("rows", "protos"), P("protos", "rows"), P("rows"))
    out_specs = P("rows", "protos")

    def on_device(features, prototypes, masked_index):
        fits = (
            n_rows % 2 == 0
            and n_rows == 8
            and n_protos > 1
            and prototypes.shape[1] % 16 == 0
            and features.shape[1] % 16 == 0
            and features.shape[1] * n_protos == prototypes.shape[1] * n_rows
            and 2 * masked_index.shape[0] == 3 * BLOCK
            and prototypes.shape[0] % (n_rows * SPLIT * 512) == 0
        )
        if fits:
            return with_kernel(n_rows, n_protos, features, prototypes, masked_index)
        return with_collectives(features, prototypes, masked_index)

    return jax.shard_map(
        on_device, mesh=mesh, in_specs=in_specs, out_specs=out_specs, check_vma=False
    )
```
